256 devices in a mesh: seq: 32 (over y, x, core), vocab: 8 (over z).
Axes of the slice: x: 4, y: 4, z: 8, core: 2. Of those that a mesh axis runs over, the one named last changes fastest.
Arguments:
- hidden: bfloat16 [3840, 4096], P('seq'), may hold values from -32 to 32
- head_weight: bfloat16 [4096, 98304], P(None, ('seq', 'vocab')), may hold values from -0.84375 to 0.84375
- labels: int32 [3840], P('seq'), may hold values from 0 to 98303
- lengths: int32 [32], replicated, may hold values from 1 to 120, 1920 in all
- pair_map: int32 [32], replicated, may hold values from 0 to 31, each once
- ref_margin: float32 [16], replicated, may hold values from -240 to 240
Outputs:
- seq_logps: float32 [32], replicated
- pair_loss: float32 [16], replicated
- z_loss: float32 [], replicated
The draws below stay inside these ranges and needn't reach their ends.
Inputs may be any that keep to these rules, and one draw needn't show every extreme that they name: The lengths sum to 1920 and the longest is exactly 120. Each response appears once; pair p compares response pair_map[2p], chosen, with response pair_map[2p+1], rejected.
All inputs are finite; a program needn't handle non-finite values.
Results may differ from the reference program's by a relative error of at most 0.0003.
Values may be sent and summed in bfloat16 or wider, within the bound.
A program may use at most 192 MiB of HBM per device.

```python
import math
import jax
import jax.numpy as jnp
import numpy as np
from jax import lax

D = 4096
VOCAB = 98304
TOK_DEV = 120
SEQS = 32
PAIRS = 16
TOKENS = 3840


def draw_hidden(key, part):
    values_out = jnp.clip(jax.random.normal(jax.random.fold_in(key, 1), (TOKENS, D), jnp.float32), -6.0, 6.0)
    return jnp.clip(values_out, -32.0, 32.0).astype(jnp.bfloat16)


def draw_head_weight(key, part):
    weight_scale = 3.0 / math.sqrt(D)
    values_out = jnp.clip(jax.random.normal(jax.random.fold_in(key, 3), (D, VOCAB), jnp.float32), -6.0, 6.0) * weight_scale
    return values_out.astype(jnp.bfloat16)


def with_ends(values, key, smallest, top_value):
    place = [jax.random.randint(jax.random.fold_in(key, axis), (), 0, length) for axis, length in enumerate(values.shape)]
    main_axis = values.shape.index(max(values.shape))
    next_to = place[:main_axis] + [(place[main_axis] + 1) % values.shape[main_axis]] + place[main_axis + 1:]
    return values.at[tuple(place)].set(smallest).at[tuple(next_to)].set(top_value)


def profile(amount, total, reach, skew):
    weights = [(1 << 20) // math.isqrt(grade ** skew) + 1 for grade in range(2, amount + 1)]
    rest, holding = total - reach - (amount - 1), [1] * (amount - 1)
    while rest > 0:
        candidates = [i for i in range(amount - 1) if holding[i] < reach]
        pool, left = sum([weights[i] for i in candidates]), rest
        for i in candidates:
            addition = min(reach - holding[i], max(1, left * weights[i] // pool), rest)
            holding[i] = holding[i] + addition
            rest = rest - addition
    return np.array([reach] + holding)


def ragged_sizes(stream_key, number_of, total, bound, lean):
    if number_of == 2:
        one = jax.random.randint(stream_key, (), max(1, total - bound), min(bound, total - 1) + 1)
        return jnp.stack([one, total - one])
    sizes = jnp.asarray(profile(number_of, total, bound, lean), jnp.int32)
    pairs = (number_of - 1) // 2
    source_of, sink = sizes[1:1 + 2 * pairs:2], sizes[2:2 + 2 * pairs:2]
    room = jnp.minimum(source_of - 1, bound - sink)
    shifted = jax.random.randint(jax.random.fold_in(stream_key, 1), (pairs,), 0, 1 << 20) % (room + 1)
    sizes = sizes.at[1:1 + 2 * pairs:2].set(source_of - shifted).at[2:2 + 2 * pairs:2].set(sink + shifted)
    return sizes[jax.random.permutation(jax.random.fold_in(stream_key, 2), number_of)]


def centred(rng, extent, deviation, most, held_as=jnp.bfloat16):
    return jnp.clip(deviation * jax.random.normal(rng, extent, jnp.float32), -most, most).astype(held_as)


def setup_inputs(seed: int = 0) -> dict:
    key_list = jax.random.split(jax.random.key(seed), 7)
    hidden = draw_hidden(jax.random.fold_in(key_list[6], 71), 0)
    head_weight = draw_head_weight(jax.random.fold_in(key_list[6], 71), 0)
    labels = with_ends(jax.random.randint(key_list[2], (TOKENS,), 0, VOCAB), jax.random.fold_in(key_list[2], 1), 0, VOCAB - 1).astype(jnp.int32)
    lengths = ragged_sizes(key_list[3], SEQS, TOKENS // 2, TOK_DEV, 2).astype(jnp.int32)
    pair_map = jax.random.permutation(key_list[4], SEQS).astype(jnp.int32)
    ref_margin = centred(key_list[5], (PAIRS,), 40.0, 240.0, jnp.float32)
    return dict(hidden=hidden, head_weight=head_weight, labels=labels, lengths=lengths, pair_map=pair_map, ref_margin=ref_margin)


pref_beta = 0.05
zloss_weight = 0.0001


def reference(hidden, head_weight, labels, lengths, pair_map, ref_margin):
    def per_sequence(seq_items):
        row_block, label_ids = seq_items
        logits = jnp.dot(row_block, head_weight, preferred_element_type=jnp.float32)
        log_norm = jax.nn.logsumexp(logits, axis=1)
        picked = jnp.take_along_axis(logits, label_ids[:, None], axis=1)[:, 0]
        return log_norm, picked

    log_norm, picked = lax.map(per_sequence, (hidden.reshape(SEQS, TOK_DEV, D), labels.reshape(SEQS, TOK_DEV)))
    live_mask = jnp.arange(TOK_DEV, dtype=jnp.int32)[None, :] < lengths[:, None]
    seq_logps = jnp.sum(jnp.where(live_mask, picked - log_norm, 0.0), axis=1)
    chosen = seq_logps[pair_map[0::2]]
    rejected = seq_logps[pair_map[1::2]]
    pair_loss = jax.nn.softplus(-pref_beta * (chosen - rejected - ref_margin))
    live_count = jnp.sum(live_mask.astype(jnp.float32))
    z_loss = zloss_weight * jnp.sum(jnp.where(live_mask, log_norm * log_norm, 0.0)) / live_count
    return seq_logps, pair_loss, z_loss
```

```python
import functools
import heapq

import jax
import jax.numpy as jnp
from jax import lax
from jax.experimental import pallas as pl
from jax.experimental.pallas import tpu as pltpu
from jax.sharding import Mesh
from jax.sharding import PartitionSpec as P

SEQ = ("seq_0", "seq_1", "seq_2")
SEQ_VOCAB = ("seq_0", "seq_1", "seq_2", "vocab")
MESH = pl.DeviceIdType.MESH

pref_beta = 0.05
zloss_weight = 0.0001

LANES = 128
UNROLL = 4
BATCH = 8
FLIGHT = 2
WIRE = 1.32
HOP = 1.1


def broadcast_tree(dims):
    nodes = [
        (a, b, c)
        for a in range(dims[0])
        for b in range(dims[1])
        for c in range(dims[2])
        if (a, b, c) != (0, 0, 0)
    ]
    choices = {}
    for node in nodes:
        ways = []
        for axis in range(3):
            at, size = node[axis], dims[axis]
            if at and at <= size // 2:
                ways.append((axis, 1))
            if at and at >= size - size // 2:
                ways.append((axis, -1))
        choices[node] = ways
    load = {}
    taken = {}
    for node in sorted(nodes, key=lambda n: (len(choices[n]), n)):
        way = min(choices[node], key=lambda w: (load.get(w, 0), w))
        taken[node] = way
        load[way] = load.get(way, 0) + 1
    moved = True
    while moved:
        moved = False
        for node in nodes:
            for way in choices[node]:
                if load.get(way, 0) + 1 < load[taken[node]]:
                    load[taken[node]] -= 1
                    load[way] = load.get(way, 0) + 1
                    taken[node] = way
                    moved = True
    return taken


def before(node, way, dims):
    place = list(node)
    place[way[0]] = (place[way[0]] - way[1]) % dims[way[0]]
    return tuple(place)


def gather_plan(dims):
    taken = broadcast_tree(dims)
    children = {}
    for node, way in taken.items():
        children.setdefault(before(node, way, dims), []).append((node, way))

    @functools.cache
    def height(node):
        return max([1 + height(child) for child, _ in children.get(node, [])], default=0)

    @functools.cache
    def weight(node):
        return 1 + sum(weight(child) for child, _ in children.get(node, []))

    ways = sorted(set(taken.values()))
    ready = {way: [] for way in ways}
    free = {way: 0.0 for way in ways}
    flying = {way: 0 for way in ways}
    events = [(0.0, 0, "arrive", (0, 0, 0))]
    count = 1
    plan = []
    while events:
        now, _, kind, item = heapq.heappop(events)
        if kind == "arrive":
            plan.append(("wait", item, None, None))
            for child, way in children.get(item, []):
                ready[way].append(child)
        else:
            flying[item] -= 1
        for way in ways:
            while ready[way] and flying[way] < FLIGHT:
                ready[way].sort(key=lambda n: (-height(n), -weight(n), n))
                child = ready[way].pop(0)
                end = max(now, free[way]) + WIRE
                free[way] = end
                flying[way] += 1
                plan.append(("send", before(child, way, dims), child, way))
                heapq.heappush(events, (end, count, "sent", way))
                heapq.heappush(events, (end + HOP, count + 1, "arrive", child))
                count += 2
    return plan


def log_one_plus(u):
    w = u / (2.0 + u)
    square = w * w
    total = jnp.full_like(w, 1.0 / 17.0)
    for odd in (15, 13, 11, 9, 7, 5, 3, 1):
        total = total * square + 1.0 / odd
    return 2.0 * w * total


def iota(shape, dim):
    return lax.broadcasted_iota(jnp.int32, shape, dim)


def scatter_scalars(ids, values):
    out = jnp.zeros(ids.shape, jnp.int32)
    for k, value in enumerate(values):
        out = jnp.where(ids == k, value, out)
    return out


def sums_before(ids, values):
    out = jnp.zeros(ids.shape, jnp.int32)
    for k, value in enumerate(values):
        out = out + jnp.where(ids > k, value, 0)
    return out


def kernel(
    dims,
    hidden_hbm,
    weight_hbm,
    labels_ref,
    lengths_ref,
    pairs_ref,
    margins_ref,
    out_ref,
    hidden,
    weight,
    parcels,
    received,
    label_row,
    labels_all,
    gathered,
    scores,
    label_place,
    stats,
    stats_in,
    merged,
    merged_in,
    sums,
    sums_in,
    load_sem,
    parcel_sem,
    label_sem,
    block_send,
    twin_send,
    block_recv,
    twin_recv,
    stat_sem,
    merged_sem,
    sums_sem,
):
    ny, nx, nz = dims
    plane = ny * nx
    seqs = lengths_ref.shape[0]
    pairs = margins_ref.shape[0]
    window = hidden.shape[0]
    slots = parcels.shape[1]
    rows = gathered.shape[2]
    columns = weight.shape[1]
    halves = plane // nz
    part_rows = rows // halves
    y, x = lax.axis_index("seq_0"), lax.axis_index("seq_1")
    core, z = lax.axis_index("seq_2"), lax.axis_index("vocab")
    here = y * nx + x
    mine = here * 2 + core
    twin = 1 - core

    def shifted(dy, dx, dz):
        return ((y + dy) % ny, (x + dx) % nx, (z + dz) % nz)

    def chip_of(node):
        cy, cx, cz = shifted(-node[0] + ny, -node[1] + nx, -node[2] + nz)
        return (cy * nx + cx) * nz + cz

    load_hidden = pltpu.make_async_copy(hidden_hbm, hidden, load_sem.at[0])
    load_weight = pltpu.make_async_copy(weight_hbm, weight, load_sem.at[1])
    load_hidden.start()
    load_weight.start()

    far = lambda n, size: min(n, size - n)
    plane_steps = sorted(
        [(a, b) for a in range(ny) for b in range(nx)],
        key=lambda s: -(far(s[0], ny) + far(s[1], nx)),
    )
    plane_peers = [(a, b, c) for a, b in plane_steps for c in (0, 1) if (a, b, c) != (0, 0, 0)]

    def peer_of(step):
        py, px, _ = shifted(step[0], step[1], 0)
        pc = twin if step[2] else core
        return py, px, pc

    barrier = pltpu.get_barrier_semaphore()
    for step in plane_peers:
        py, px, pc = peer_of(step)
        pl.semaphore_signal(barrier, inc=1, device_id=(py, px, pc, z), device_id_type=MESH)
    z_steps = sorted({1 % nz, nz - 1} - {0})
    for dz in z_steps:
        pl.semaphore_signal(
            barrier, inc=1, device_id=(y, x, core, (z + dz) % nz), device_id_type=MESH
        )

    lens = [lengths_ref[s] for s in range(seqs)]
    slot_ids = iota((1, seqs * slots), 1)
    slot_seq = slot_ids // slots
    first = sums_before(slot_seq, lens)
    place = nz * (slot_ids % slots) + ((z - first) & (nz - 1))
    row_of_slot = jnp.where(
        place < scatter_scalars(slot_seq, lens), (first + place - z) // nz, -1
    )
    own_first = jnp.int32(0)
    for s in range(seqs - 1):
        own_first = own_first + jnp.where(mine > s, lens[s], 0)
    own_place = nz * iota((slots, window), 0) + ((z - own_first) & (nz - 1))
    choose = jnp.where(own_place == iota((slots, window), 1), 1.0, 0.0).astype(jnp.bfloat16)

    label_row[...] = jnp.zeros(label_row.shape, jnp.int32)
    label_row[0:1, 0:window] = labels_ref[...]
    labels_all[mine] = label_row[...]
    scores[...] = jnp.zeros(scores.shape, jnp.float32)
    load_hidden.wait()
    chosen = jnp.dot(choose, hidden[...], preferred_element_type=jnp.float32)
    chosen = chosen.astype(jnp.bfloat16)
    for j in range(2 * plane):
        parcels[j] = chosen[:, j * LANES : (j + 1) * LANES]
    received[mine] = parcels[mine]

    pl.semaphore_wait(barrier, len(plane_peers) + len(z_steps))

    for step in plane_peers:
        py, px, pc = peer_of(step)
        pltpu.make_async_remote_copy(
            src_ref=parcels.at[(py * nx + px) * 2 + pc],
            dst_ref=received.at[mine],
            send_sem=parcel_sem.at[0],
            recv_sem=parcel_sem.at[1],
            device_id=(py, px, pc, z),
            device_id_type=MESH,
        ).start()
    for step in plane_peers:
        py, px, pc = peer_of(step)
        pltpu.make_async_remote_copy(
            src_ref=label_row,
            dst_ref=labels_all.at[mine],
            send_sem=label_sem.at[0],
            recv_sem=label_sem.at[1],
            device_id=(py, px, pc, z),
            device_id_type=MESH,
        ).start()
    compact = jnp.where(iota((rows, seqs * slots), 0) == row_of_slot, 1.0, 0.0)
    compact = compact.astype(jnp.bfloat16)
    others = received.at[pl.ds(0, 2 * plane - 1)]
    pltpu.make_async_copy(others, others, parcel_sem.at[1]).wait()
    block = jnp.dot(
        compact,
        received[...].reshape(seqs * slots, LANES),
        preferred_element_type=jnp.float32,
    )
    own_chip = here * nz + z
    gathered[core, own_chip] = block.astype(jnp.bfloat16)

    lane = iota((1, LANES), 1)
    lane_first = sums_before(lane, lens)
    lane_len = scatter_scalars(lane, lens)
    sub = iota((LANES, LANES), 0)
    sub_first = sums_before(sub, lens)
    sub_len = scatter_scalars(sub, lens)

    def label_table():
        row_ids = iota((LANES, LANES), 0)
        table = jnp.zeros((LANES, LANES), jnp.int32)
        for s in range(seqs):
            table = jnp.where(row_ids == s, labels_all[s], table)
        col_first = (mine * nz + z) * columns
        local = table - col_first
        code = jnp.where((local >= 0) & (local < columns), local + 1, 0)
        pieces = [code // 16, code % 16, sub_first // 16, sub_first % 16]
        return [piece.astype(jnp.float32).astype(jnp.bfloat16) for piece in pieces]

    def place_labels(pieces, zz):
        ids = nz * iota((rows, LANES), 0) + zz
        member = (ids >= lane_first) & (ids < lane_first + lane_len)
        member = jnp.where(member, 1.0, 0.0).astype(jnp.bfloat16)
        high, low, first_high, first_low = [
            jnp.dot(member, piece, preferred_element_type=jnp.float32) for piece in pieces
        ]
        position = ids.astype(jnp.float32) - (16.0 * first_high + first_low)
        at = position == iota((rows, LANES), 1).astype(jnp.float32)
        code = jnp.sum(jnp.where(at, 16.0 * high + low, 0.0), axis=1, keepdims=True)
        label_place[zz] = jnp.broadcast_to(code - 1.0, (rows, LANES))

    def multiply(chips):
        def body(turn, _):
            products = []
            for u in range(UNROLL):
                chip = chips[u]
                for t in range(1, len(chips) // UNROLL):
                    chip = jnp.where(turn == t, chips[t * UNROLL + u], chip)
                depth = pl.multiple_of((chip // nz) * (2 * LANES), 2 * LANES)
                pair = jnp.concatenate([gathered[0, chip], gathered[1, chip]], axis=1)
                products.append(
                    (
                        chip % nz,
                        jnp.dot(
                            pair,
                            weight[pl.ds(depth, 2 * LANES), :],
                            preferred_element_type=jnp.float32,
                        ),
                    )
                )
            for zz, product in products:
                scores[zz] = scores[zz] + product
            return 0

        lax.fori_loop(0, len(chips) // UNROLL, body, 0)

    plan = gather_plan(dims)
    order = {}
    for kind, node, _, _ in plan:
        if kind == "wait":
            order[node] = len(order)
    nodes = list(order)
    done = 0
    sites = 0
    pieces = None

    def wait_twin(k):
        chip = chip_of(nodes[k])
        ref = gathered.at[twin, chip]
        pltpu.make_async_copy(ref, ref, twin_recv.at[k]).wait()

    def compute(upto):
        nonlocal done, sites, pieces
        while done < upto:
            take = min(BATCH, upto - done)
            if done == 0:
                load_weight.wait()
            for k in range(done, done + take):
                wait_twin(k)
            multiply([chip_of(nodes[k]) for k in range(done, done + take)])
            if pieces is None:
                other_labels = labels_all.at[pl.ds(0, 2 * plane - 1)]
                pltpu.make_async_copy(other_labels, other_labels, label_sem.at[1]).wait()
                pieces = label_table()
            if sites < nz:
                place_labels(pieces, sites)
            done += take
            sites += 1

    for kind, node, child, way in plan:
        chip = chip_of(node)
        ref = gathered.at[core, chip]
        if kind == "wait":
            k = order[node]
            if k:
                pltpu.make_async_copy(ref, ref, block_recv.at[k]).wait()
            pltpu.make_async_remote_copy(
                src_ref=ref,
                dst_ref=ref,
                send_sem=twin_send,
                recv_sem=twin_recv.at[k],
                device_id=(y, x, twin, z),
                device_id_type=MESH,
            ).start()
            ready = k + 1 - BATCH
            if ready > done and ready - done >= BATCH:
                compute(done + BATCH)
        else:
            step = [0, 0, 0]
            step[way[0]] = way[1] % dims[way[0]]
            ty, tx, tz = shifted(*step)
            pltpu.make_async_remote_copy(
                src_ref=ref,
                dst_ref=ref,
                send_sem=block_send,
                recv_sem=block_recv.at[order[child]],
                device_id=(ty, tx, core, tz),
                device_id_type=MESH,
            ).start()
    compute(len(nodes))
    while sites < nz:
        place_labels(pieces, sites)
        sites += 1

    column_ids = iota((part_rows, columns), 1).astype(jnp.float32)
    spot = iota((part_rows, LANES), 1)
    for j in range(plane):
        zz, start = j // halves, (j % halves) * part_rows
        part = scores[zz, start : start + part_rows, :]
        code = label_place[zz, start : start + part_rows, 0:1]
        top = jnp.max(part, axis=1, keepdims=True)
        total = jnp.sum(jnp.exp(part - top), axis=1, keepdims=True)
        picked = jnp.sum(jnp.where(column_ids == code, part, 0.0), axis=1, keepdims=True)
        packed = jnp.where(
            spot == 0, top, jnp.where(spot == 1, total, jnp.where(spot == 2, picked, 0.0))
        )
        if part_rows < LANES:
            packed = jnp.concatenate(
                [packed, jnp.zeros((LANES - part_rows, LANES), jnp.float32)], axis=0
            )
        stats[j] = packed.T[0:4, :]

    plane_chips = [s for s in plane_steps if s != (0, 0)]
    stats_in[here] = stats[here]
    for a, b in plane_chips:
        py, px, _ = shifted(a, b, 0)
        pltpu.make_async_remote_copy(
            src_ref=stats.at[py * nx + px],
            dst_ref=stats_in.at[here],
            send_sem=stat_sem.at[0],
            recv_sem=stat_sem.at[1],
            device_id=(py, px, core, z),
            device_id_type=MESH,
        ).start()
    other_stats = stats_in.at[pl.ds(0, plane - 1)]
    pltpu.make_async_copy(other_stats, other_stats, stat_sem.at[1]).wait()

    def merge(ref, count):
        tops = [ref[k, 0:1, :] for k in range(count)]
        top = functools.reduce(jnp.maximum, tops)
        total = functools.reduce(
            jnp.add, [ref[k, 1:2, :] * jnp.exp(tops[k] - top) for k in range(count)]
        )
        picked = functools.reduce(jnp.add, [ref[k, 2:3, :] for k in range(count)])
        return top, total, picked

    top, total, picked = merge(stats_in, plane)
    merged[0:1, :] = top
    merged[1:2, :] = total
    merged[2:3, :] = picked
    merged[3:4, :] = jnp.zeros((1, LANES), jnp.float32)
    line = z * 2 + core
    merged_in[line] = merged[...]
    line_peers = sorted(
        [(dz, dc) for dz in range(nz) for dc in (0, 1) if (dz, dc) != (0, 0)],
        key=lambda s: -far(s[0], nz),
    )
    for dz, dc in line_peers:
        pltpu.make_async_remote_copy(
            src_ref=merged,
            dst_ref=merged_in.at[line],
            send_sem=merged_sem.at[0],
            recv_sem=merged_sem.at[1],
            device_id=(y, x, twin if dc else core, (z + dz) % nz),
            device_id_type=MESH,
        ).start()
    other_merged = merged_in.at[pl.ds(0, 2 * nz - 1)]
    pltpu.make_async_copy(other_merged, other_merged, merged_sem.at[1]).wait()

    top, total, picked = merge(merged_in, 2 * nz)
    filled = lane < part_rows
    log_norm = top + jnp.log(jnp.where(filled, total, 1.0))
    gain = jnp.where(filled, picked - log_norm, 0.0)
    row_ids = nz * ((here % halves) * part_rows + lane) + here // halves
    inside = (row_ids >= sub_first) & (row_ids < sub_first + sub_len)
    inside = jnp.where(inside, 1.0, 0.0)
    contract = (((1,), (1,)), ((), ()))
    by_seq = lax.dot_general(
        jnp.broadcast_to(gain, (8, LANES)),
        inside,
        contract,
        precision=lax.Precision.HIGHEST,
        preferred_element_type=jnp.float32,
    )[0:1, :]
    squares = jnp.sum(jnp.where(filled, log_norm * log_norm, 0.0), axis=1, keepdims=True)
    sums[...] = jnp.where(lane == seqs, squares, by_seq)
    sums_in[here] = sums[...]
    for a, b in plane_chips:
        py, px, _ = shifted(a, b, 0)
        pltpu.make_async_remote_copy(
            src_ref=sums,
            dst_ref=sums_in.at[here],
            send_sem=sums_sem.at[0],
            recv_sem=sums_sem.at[1],
            device_id=(py, px, core, z),
            device_id_type=MESH,
        ).start()
    pair_ids = iota((LANES, LANES), 0)
    select = jnp.zeros((LANES, LANES), jnp.float32)
    seq_ids = iota((LANES, LANES), 1)
    margins = jnp.zeros((1, LANES), jnp.float32)
    for p in range(pairs):
        hit = jnp.where(seq_ids == pairs_ref[2 * p], 1.0, 0.0)
        hit = hit - jnp.where(seq_ids == pairs_ref[2 * p + 1], 1.0, 0.0)
        select = jnp.where(pair_ids == p, hit, select)
        margins = jnp.where(lane == p, margins_ref[p], margins)
    live = functools.reduce(jnp.add, lens).astype(jnp.float32)

    def drain(ref, sem):
        pltpu.make_async_copy(ref, ref, sem).wait()

    drain(others, parcel_sem.at[0])
    drain(labels_all.at[pl.ds(0, 2 * plane - 1)], label_sem.at[0])
    drain(gathered.at[0, pl.ds(0, plane * nz - 1)], block_send)
    drain(gathered.at[0], twin_send)
    drain(other_stats, stat_sem.at[0])
    drain(other_merged, merged_sem.at[0])
    other_sums = sums_in.at[pl.ds(0, plane - 1)]
    drain(other_sums, sums_sem.at[1])

    row = functools.reduce(jnp.add, [sums_in[k] for k in range(plane)])
    seq_row = jnp.where(lane < seqs, row, 0.0)
    difference = lax.dot_general(
        jnp.broadcast_to(seq_row, (8, LANES)),
        select,
        contract,
        precision=lax.Precision.HIGHEST,
        preferred_element_type=jnp.float32,
    )[0:1, :]
    score = -pref_beta * (difference - margins)
    pair_row = jnp.maximum(score, 0.0) + log_one_plus(jnp.exp(-jnp.abs(score)))
    z_row = zloss_weight * row / live
    out_ref[0:1, :] = seq_row
    out_ref[1:2, :] = pair_row
    out_ref[2:3, :] = z_row
    out_ref[3:8, :] = jnp.zeros((5, LANES), jnp.float32)
    drain(other_sums, sums_sem.at[0])


def per_device(dims, hidden, head_weight, labels, lengths, pair_map, ref_margin):
    ny, nx, nz = dims
    plane = ny * nx
    window, width = hidden.shape
    columns = head_weight.shape[1]
    seqs = lengths.shape[0]
    live = seqs * window // 2
    rows = live // nz
    slots = -(-window // (nz * 16)) * 16
    bf16, f32, i32 = jnp.bfloat16, jnp.float32, jnp.int32
    vmem = pltpu.VMEM
    dma = pltpu.SemaphoreType.DMA
    out = pl.pallas_call(
        functools.partial(kernel, dims),
        out_shape=jax.ShapeDtypeStruct((8, LANES), f32),
        in_specs=[
            pl.BlockSpec(memory_space=pl.ANY),
            pl.BlockSpec(memory_space=pl.ANY),
            pl.BlockSpec(memory_space=vmem),
            pl.BlockSpec(memory_space=pltpu.SMEM),
            pl.BlockSpec(memory_space=pltpu.SMEM),
            pl.BlockSpec(memory_space=pltpu.SMEM),
        ],
        out_specs=pl.BlockSpec(memory_space=vmem),
        scratch_shapes=[
            vmem((window, width), bf16),
            vmem((width, columns), bf16),
            vmem((2 * plane, slots, LANES), bf16),
            vmem((2 * plane, slots, LANES), bf16),
            vmem((1, LANES), i32),
            vmem((2 * plane, 1, LANES), i32),
            vmem((2, plane * nz, rows, LANES), bf16),
            vmem((nz, rows, columns), f32),
            vmem((nz, rows, LANES), f32),
            vmem((plane, 4, LANES), f32),
            vmem((plane, 4, LANES), f32),
            vmem((4, LANES), f32),
            vmem((2 * nz, 4, LANES), f32),
            vmem((1, LANES), f32),
            vmem((plane, 1, LANES), f32),
            dma((2,)),
            dma((2,)),
            dma((2,)),
            dma(()),
            dma(()),
            dma((plane * nz,)),
            dma((plane * nz,)),
            dma((2,)),
            dma((2,)),
            dma((2,)),
        ],
        compiler_params=pltpu.CompilerParams(collective_id=0, has_side_effects=True),
    )(hidden, head_weight, labels.reshape(1, window), lengths, pair_map, ref_margin)
    return out[0, :seqs], out[1, : seqs // 2], out[2, seqs]


def solution(mesh):
    nz = mesh.shape["vocab"]
    ny = nx = {32: 4, 8: 2}[mesh.shape["seq"]]
    torus = Mesh(
        mesh.devices.reshape(ny, nx, 2, nz), ("seq_0", "seq_1", "seq_2", "vocab")
    )
    return jax.shard_map(
        functools.partial(per_device, (ny, nx, nz)),
        mesh=torus,
        in_specs=(P(SEQ, None), P(None, SEQ_VOCAB), P(SEQ), P(), P(), P()),
        out_specs=(P(), P(), P()),
        check_vma=False,
    )
```

```python
import functools
import heapq
import math

import jax
import jax.numpy as jnp
from jax import lax
from jax.experimental import pallas as pl
from jax.experimental.pallas import tpu as pltpu
from jax.sharding import Mesh
from jax.sharding import PartitionSpec as P

SEQ = ("seq_0", "seq_1", "seq_2")
SEQ_VOCAB = ("seq_0", "seq_1", "seq_2", "vocab")
MESH = pl.DeviceIdType.MESH

pref_beta = 0.05
zloss_weight = 0.0001

LANES = 128
CHUNK = 4
CUTS = 2
BACKLOG = 1.8
WIRE = 1.33
HOP = 2.2
TWIN = 1.6
ISSUE = 0.012
PAIR = 0.108
PLACE = 0.35

STEPS = [(0, 1), (0, -1), (1, 1), (1, -1), (2, 1), (2, -1)]
WAYS = [
    4, 4, 4, 5, 5, 5, 5, 2, 2, 4, 4, 4, 2, 2, 2, 3, 4, 2, 3, 5, 2, 3, 5, 3, 4, 3, 3, 3, 5, 3, 3, 0,
    0, 4, 0, 4, 0, 5, 0, 0, 4, 0, 2, 0, 5, 0, 0, 0, 2, 2, 0, 2, 3, 3, 3, 3, 0, 3, 4, 3, 5, 0, 5, 1,
    0, 4, 0, 0, 5, 0, 1, 1, 1, 0, 2, 1, 5, 0, 2, 3, 4, 4, 3, 2, 5, 1, 0, 1, 1, 4, 4, 5, 5, 5, 3, 1,
    1, 4, 1, 5, 1, 1, 5, 2, 4, 1, 1, 2, 2, 1, 2, 2, 1, 2, 2, 2, 1, 5, 1, 1, 1, 3, 4, 4, 3, 5, 3,
]


def broadcast_tree(dims):
    nodes = [
        (a, b, c)
        for a in range(dims[0])
        for b in range(dims[1])
        for c in range(dims[2])
        if (a, b, c) != (0, 0, 0)
    ]
    if len(nodes) == len(WAYS):
        return {node: STEPS[way] for node, way in zip(nodes, WAYS)}
    taken = {}
    for node in nodes:
        axis = next(k for k in range(3) if node[k])
        taken[node] = (axis, 1 if node[axis] <= dims[axis] // 2 else -1)
    return taken


def before(node, way, dims):
    place = list(node)
    place[way[0]] = (place[way[0]] - way[1]) % dims[way[0]]
    return tuple(place)


def gather_plan(dims, cuts, places):
    taken = broadcast_tree(dims)
    children = {}
    for node, way in taken.items():
        children.setdefault(before(node, way, dims), []).append((node, way))

    @functools.cache
    def height(node):
        return max([1 + height(child) for child, _ in children.get(node, [])], default=0)

    @functools.cache
    def weight(node):
        return 1 + sum(weight(child) for child, _ in children.get(node, []))

    wire = WIRE / cuts
    ways = sorted(set(taken.values()))
    ready = {way: [] for way in ways}
    free = {way: 0.0 for way in ways}
    left = {way: cuts * sum(w == way for w in taken.values()) for way in ways}
    arrivals = [(0.0, cut, ((0, 0, 0), cut)) for cut in range(cuts)]
    count = cuts
    now = 0.0
    plan = []
    arrived = {}
    waiting = {}
    placed = 0
    multiplied = 0
    cost = PAIR * CHUNK

    def multiply(nodes):
        plan.append(("multiply", tuple(nodes), None, None))
        for node in nodes:
            del waiting[node]

    while arrivals or waiting:
        while arrivals and arrivals[0][0] <= now:
            piece = heapq.heappop(arrivals)[2]
            node, cut = piece
            plan.append(("wait", piece, None, None))
            now += ISSUE
            for child, way in children.get(node, []):
                ready[way].append((child, cut))
            arrived[node] = arrived.get(node, 0) + 1
            if arrived[node] == cuts:
                plan.append(("twin", node, None, None))
                now += ISSUE
                waiting[node] = now + TWIN
        for way in ways:
            while ready[way] and free[way] - now < BACKLOG - 0.5 * wire:
                ready[way].sort(key=lambda p: (-height(p[0]), -weight(p[0]), p[1], p[0]))
                piece = ready[way].pop(0)
                free[way] = max(now, free[way]) + wire
                left[way] -= 1
                plan.append(("send", (before(piece[0], way, dims), piece[1]), piece, way))
                now += ISSUE
                heapq.heappush(arrivals, (free[way] + HOP, count, piece))
                count += 1
        if arrivals and arrivals[0][0] <= now:
            continue
        coming = arrivals[0][0] if arrivals else math.inf
        queued = min([free[way] - now for way in ways if left[way]], default=math.inf)
        there = [node for node, when in waiting.items() if when <= now]
        if len(there) >= CHUNK and (queued >= cost or coming >= now + cost or len(waiting) > 32):
            multiply(there[:CHUNK])
            multiplied += CHUNK
            now += cost
            continue
        if placed < places and multiplied >= 2 * CHUNK:
            if queued >= PLACE or coming >= now + PLACE:
                plan.append(("place", placed, None, None))
                placed += 1
                now += PLACE
                continue
        later = [coming]
        later += [free[way] - BACKLOG + 0.5 * wire for way in ways if ready[way]]
        if len(waiting) >= CHUNK:
            later.append(max(sorted(waiting.values())[CHUNK - 1], now + 0.05))
        if min(later) == math.inf:
            multiply(list(waiting)[:CHUNK])
            now += cost
            continue
        now = max(now + 1e-6, min(later))
    for k in range(placed, places):
        plan.append(("place", k, None, None))
    return plan


def log_one_plus(u):
    w = u / (2.0 + u)
    square = w * w
    total = jnp.full_like(w, 1.0 / 17.0)
    for odd in (15, 13, 11, 9, 7, 5, 3, 1):
        total = total * square + 1.0 / odd
    return 2.0 * w * total


def iota(shape, dim):
    return lax.broadcasted_iota(jnp.int32, shape, dim)


def scatter_scalars(ids, values):
    out = jnp.zeros(ids.shape, jnp.int32)
    for k, value in enumerate(values):
        out = jnp.where(ids == k, value, out)
    return out


def sums_before(ids, values):
    out = jnp.zeros(ids.shape, jnp.int32)
    for k, value in enumerate(values):
        out = out + jnp.where(ids > k, value, 0)
    return out


def kernel(
    dims,
    hidden_hbm,
    weight_hbm,
    labels_ref,
    lengths_ref,
    pairs_ref,
    margins_ref,
    seq_out,
    pair_out,
    z_out,
    hidden,
    weight,
    parcels,
    received,
    label_row,
    labels_all,
    gathered,
    scores,
    label_place,
    packed,
    stats,
    stats_in,
    merged,
    merged_in,
    sums,
    sums_in,
    load_sem,
    parcel_sem,
    label_sem,
    block_send,
    twin_send,
    block_recv,
    twin_recv,
    stat_sem,
    merged_sem,
    sums_sem,
):
    ny, nx, nz = dims
    plane = ny * nx
    seqs = lengths_ref.shape[0]
    pairs = margins_ref.shape[0]
    window = hidden.shape[0]
    slots = parcels.shape[1]
    rows = gathered.shape[2]
    columns = weight.shape[1]
    halves = plane // nz
    part_rows = rows // halves
    y, x = lax.axis_index("seq_0"), lax.axis_index("seq_1")
    core, z = lax.axis_index("seq_2"), lax.axis_index("vocab")
    here = y * nx + x
    mine = here * 2 + core
    twin = 1 - core

    def shifted(dy, dx, dz):
        return ((y + dy) % ny, (x + dx) % nx, (z + dz) % nz)

    def chip_of(node):
        cy, cx, cz = shifted(-node[0] + ny, -node[1] + nx, -node[2] + nz)
        return (cy * nx + cx) * nz + cz

    far = lambda n, size: min(n, size - n)
    plane_steps = sorted(
        [(a, b) for a in range(ny) for b in range(nx)],
        key=lambda s: -(far(s[0], ny) + far(s[1], nx)),
    )
    plane_peers = [(a, b, c) for a, b in plane_steps for c in (0, 1) if (a, b, c) != (0, 0, 0)]

    def peer_of(step):
        py, px, _ = shifted(step[0], step[1], 0)
        pc = twin if step[2] else core
        return py, px, pc

    barrier = pltpu.get_barrier_semaphore()
    for step in plane_peers:
        py, px, pc = peer_of(step)
        pl.semaphore_signal(barrier, inc=1, device_id=(py, px, pc, z), device_id_type=MESH)
    z_steps = sorted({1 % nz, nz - 1} - {0})
    for dz in z_steps:
        pl.semaphore_signal(
            barrier, inc=1, device_id=(y, x, core, (z + dz) % nz), device_id_type=MESH
        )

    load_hidden = pltpu.make_async_copy(hidden_hbm, hidden, load_sem.at[0])
    load_weight = pltpu.make_async_copy(weight_hbm, weight, load_sem.at[1])
    load_hidden.start()

    lens = [lengths_ref[s] for s in range(seqs)]
    own_first = jnp.int32(0)
    for s in range(seqs - 1):
        own_first = own_first + jnp.where(mine > s, lens[s], 0)
    own_place = nz * iota((slots, window), 0) + ((z - own_first) & (nz - 1))
    choose = jnp.where(own_place == iota((slots, window), 1), 1.0, 0.0).astype(jnp.bfloat16)

    label_row[...] = jnp.zeros(label_row.shape, jnp.int32)
    label_row[0:1, 0:window] = labels_ref[...]
    labels_all[mine] = label_row[...]
    load_hidden.wait()
    load_weight.start()
    chosen = jnp.dot(choose, hidden[...], preferred_element_type=jnp.float32)
    chosen = chosen.astype(jnp.bfloat16)
    for j in range(2 * plane):
        parcels[j] = chosen[:, j * LANES : (j + 1) * LANES]
    received[mine] = parcels[mine]

    pl.semaphore_wait(barrier, len(plane_peers) + len(z_steps))

    for step in plane_peers:
        py, px, pc = peer_of(step)
        pltpu.make_async_remote_copy(
            src_ref=parcels.at[(py * nx + px) * 2 + pc],
            dst_ref=received.at[mine],
            send_sem=parcel_sem.at[0],
            recv_sem=parcel_sem.at[1],
            device_id=(py, px, pc, z),
            device_id_type=MESH,
        ).start()
    for step in plane_peers:
        py, px, pc = peer_of(step)
        pltpu.make_async_remote_copy(
            src_ref=label_row,
            dst_ref=labels_all.at[mine],
            send_sem=label_sem.at[0],
            recv_sem=label_sem.at[1],
            device_id=(py, px, pc, z),
            device_id_type=MESH,
        ).start()
    slot_ids = iota((1, seqs * slots), 1)
    slot_seq = slot_ids // slots
    first = sums_before(slot_seq, lens)
    place = nz * (slot_ids % slots) + ((z - first) & (nz - 1))
    row_of_slot = jnp.where(
        place < scatter_scalars(slot_seq, lens), (first + place - z) // nz, -1
    )
    scores[...] = jnp.zeros(scores.shape, jnp.float32)
    compact = jnp.where(iota((rows, seqs * slots), 0) == row_of_slot, 1.0, 0.0)
    compact = compact.astype(jnp.bfloat16)
    others = received.at[pl.ds(0, 2 * plane - 1)]
    pltpu.make_async_copy(others, others, parcel_sem.at[1]).wait()
    block = jnp.dot(
        compact,
        received[...].reshape(seqs * slots, LANES),
        preferred_element_type=jnp.float32,
    )
    own_chip = here * nz + z
    gathered[core, own_chip] = block.astype(jnp.bfloat16)

    lane = iota((1, LANES), 1)
    lane_first = sums_before(lane, lens)
    lane_len = scatter_scalars(lane, lens)
    sub = iota((LANES, LANES), 0)
    sub_first = sums_before(sub, lens)
    sub_len = scatter_scalars(sub, lens)

    def label_table():
        row_ids = iota((LANES, LANES), 0)
        table = jnp.zeros((LANES, LANES), jnp.int32)
        for s in range(seqs):
            table = jnp.where(row_ids == s, labels_all[s], table)
        col_first = (mine * nz + z) * columns
        local = table - col_first
        code = jnp.where((local >= 0) & (local < columns), local + 1, 0)
        pieces = [code // 16, code % 16, sub_first // 16, sub_first % 16]
        return [piece.astype(jnp.float32).astype(jnp.bfloat16) for piece in pieces]

    def place_labels(pieces, zz):
        ids = nz * iota((rows, LANES), 0) + zz
        member = (ids >= lane_first) & (ids < lane_first + lane_len)
        member = jnp.where(member, 1.0, 0.0).astype(jnp.bfloat16)
        high, low, first_high, first_low = [
            jnp.dot(member, piece, preferred_element_type=jnp.float32) for piece in pieces
        ]
        position = ids.astype(jnp.float32) - (16.0 * first_high + first_low)
        at = position == iota((rows, LANES), 1).astype(jnp.float32)
        code = jnp.sum(jnp.where(at, 16.0 * high + low, 0.0), axis=1, keepdims=True)
        label_place[zz] = jnp.broadcast_to(code - 1.0, (rows, LANES))

    def multiply(chips):
        products = []
        for chip in chips:
            depth = pl.multiple_of((chip // nz) * (2 * LANES), 2 * LANES)
            pair = jnp.concatenate([gathered[0, chip], gathered[1, chip]], axis=1)
            product = jnp.dot(
                pair, weight[pl.ds(depth, 2 * LANES), :], preferred_element_type=jnp.float32
            )
            products.append((chip % nz, product))
        for zz, product in products:
            scores[zz] = scores[zz] + product

    edges = [0, LANES, rows] if CUTS == 2 else [0, rows]
    plan = gather_plan(dims, CUTS, nz)
    order = {}
    for kind, item, _, _ in plan:
        if kind == "twin":
            order[item] = len(order)

    def piece_ref(node, cut):
        return gathered.at[core, chip_of(node), pl.ds(edges[cut], edges[cut + 1] - edges[cut])]

    def drain(ref, sem):
        pltpu.make_async_copy(ref, ref, sem).wait()

    pieces = None
    first_product = True
    for kind, item, child, way in plan:
        if kind == "wait":
            node, cut = item
            if node != (0, 0, 0):
                drain(piece_ref(node, cut), block_recv.at[order[node] * CUTS + cut])
        elif kind == "twin":
            ref = gathered.at[core, chip_of(item)]
            pltpu.make_async_remote_copy(
                src_ref=ref,
                dst_ref=ref,
                send_sem=twin_send,
                recv_sem=twin_recv.at[order[item]],
                device_id=(y, x, twin, z),
                device_id_type=MESH,
            ).start()
        elif kind == "send":
            node, cut = item
            ref = piece_ref(node, cut)
            step = [0, 0, 0]
            step[way[0]] = way[1] % dims[way[0]]
            ty, tx, tz = shifted(*step)
            pltpu.make_async_remote_copy(
                src_ref=ref,
                dst_ref=ref,
                send_sem=block_send,
                recv_sem=block_recv.at[order[child[0]] * CUTS + cut],
                device_id=(ty, tx, core, tz),
                device_id_type=MESH,
            ).start()
        elif kind == "multiply":
            if first_product:
                load_weight.wait()
                first_product = False
            for node in item:
                drain(gathered.at[twin, chip_of(node)], twin_recv.at[order[node]])
            multiply([chip_of(node) for node in item])
        else:
            if pieces is None:
                drain(labels_all.at[pl.ds(0, 2 * plane - 1)], label_sem.at[1])
                pieces = label_table()
            place_labels(pieces, item)

    column_ids = iota((rows, columns), 1).astype(jnp.float32)
    spot = iota((rows, LANES), 1)
    for zz in range(nz):
        top = jnp.max(scores[zz], axis=1, keepdims=True)
        packed[zz, 0:rows, :] = jnp.broadcast_to(top, (rows, LANES))
    for zz in range(nz):
        part = scores[zz]
        top = packed[zz, 0:rows, 0:1]
        total = jnp.sum(jnp.exp(part - top), axis=1, keepdims=True)
        hit = column_ids == label_place[zz, :, 0:1]
        picked = jnp.sum(jnp.where(hit, part, 0.0), axis=1, keepdims=True)
        packed[zz, 0:rows, :] = jnp.where(spot == 0, top, jnp.where(spot == 1, total, picked))
        packed[zz, rows:, :] = jnp.zeros((LANES - part_rows, LANES), jnp.float32)
    for j in range(plane):
        start = (j % halves) * part_rows
        stats[j] = packed[j // halves, start : start + LANES, :].T[0:4, :]

    plane_chips = [s for s in plane_steps if s != (0, 0)]
    stats_in[here] = stats[here]
    for a, b in plane_chips:
        py, px, _ = shifted(a, b, 0)
        pltpu.make_async_remote_copy(
            src_ref=stats.at[py * nx + px],
            dst_ref=stats_in.at[here],
            send_sem=stat_sem.at[0],
            recv_sem=stat_sem.at[1],
            device_id=(py, px, core, z),
            device_id_type=MESH,
        ).start()
    other_stats = stats_in.at[pl.ds(0, plane - 1)]
    pltpu.make_async_copy(other_stats, other_stats, stat_sem.at[1]).wait()

    def merge(ref, count):
        tops = [ref[k, 0:1, :] for k in range(count)]
        top = functools.reduce(jnp.maximum, tops)
        total = functools.reduce(
            jnp.add, [ref[k, 1:2, :] * jnp.exp(tops[k] - top) for k in range(count)]
        )
        picked = functools.reduce(jnp.add, [ref[k, 2:3, :] for k in range(count)])
        return top, total, picked

    top, total, picked = merge(stats_in, plane)
    merged[0:1, :] = top
    merged[1:2, :] = total
    merged[2:3, :] = picked
    merged[3:4, :] = jnp.zeros((1, LANES), jnp.float32)
    line = z * 2 + core
    merged_in[line] = merged[...]
    line_peers = sorted(
        [(dz, dc) for dz in range(nz) for dc in (0, 1) if (dz, dc) != (0, 0)],
        key=lambda s: -far(s[0], nz),
    )
    for dz, dc in line_peers:
        pltpu.make_async_remote_copy(
            src_ref=merged,
            dst_ref=merged_in.at[line],
            send_sem=merged_sem.at[0],
            recv_sem=merged_sem.at[1],
            device_id=(y, x, twin if dc else core, (z + dz) % nz),
            device_id_type=MESH,
        ).start()
    other_merged = merged_in.at[pl.ds(0, 2 * nz - 1)]
    pltpu.make_async_copy(other_merged, other_merged, merged_sem.at[1]).wait()

    top, total, picked = merge(merged_in, 2 * nz)
    filled = lane < part_rows
    log_norm = top + jnp.log(jnp.where(filled, total, 1.0))
    gain = jnp.where(filled, picked - log_norm, 0.0)
    row_ids = nz * ((here % halves) * part_rows + lane) + here // halves
    inside = (row_ids >= sub_first) & (row_ids < sub_first + sub_len)
    inside = jnp.where(inside, 1.0, 0.0)
    contract = (((1,), (1,)), ((), ()))
    by_seq = lax.dot_general(
        jnp.broadcast_to(gain, (8, LANES)),
        inside,
        contract,
        precision=lax.Precision.HIGHEST,
        preferred_element_type=jnp.float32,
    )[0:1, :]
    squares = jnp.sum(jnp.where(filled, log_norm * log_norm, 0.0), axis=1, keepdims=True)
    sums[...] = jnp.where(lane == seqs, squares, by_seq)
    sums_in[here] = sums[...]
    for a, b in plane_chips:
        py, px, _ = shifted(a, b, 0)
        pltpu.make_async_remote_copy(
            src_ref=sums,
            dst_ref=sums_in.at[here],
            send_sem=sums_sem.at[0],
            recv_sem=sums_sem.at[1],
            device_id=(py, px, core, z),
            device_id_type=MESH,
        ).start()
    pair_ids = iota((LANES, LANES), 0)
    select = jnp.zeros((LANES, LANES), jnp.float32)
    seq_ids = iota((LANES, LANES), 1)
    margins = jnp.zeros((1, LANES), jnp.float32)
    for p in range(pairs):
        hit = jnp.where(seq_ids == pairs_ref[2 * p], 1.0, 0.0)
        hit = hit - jnp.where(seq_ids == pairs_ref[2 * p + 1], 1.0, 0.0)
        select = jnp.where(pair_ids == p, hit, select)
        margins = jnp.where(lane == p, margins_ref[p], margins)
    live = functools.reduce(jnp.add, lens).astype(jnp.float32)

    drain(others, parcel_sem.at[0])
    drain(labels_all.at[pl.ds(0, 2 * plane - 1)], label_sem.at[0])
    drain(gathered.at[0, pl.ds(0, plane * nz - 1)], block_send)
    drain(gathered.at[0], twin_send)
    drain(other_stats, stat_sem.at[0])
    drain(other_merged, merged_sem.at[0])
    other_sums = sums_in.at[pl.ds(0, plane - 1)]
    drain(other_sums, sums_sem.at[1])

    row = functools.reduce(jnp.add, [sums_in[k] for k in range(plane)])
    seq_row = jnp.where(lane < seqs, row, 0.0)
    difference = lax.dot_general(
        jnp.broadcast_to(seq_row, (8, LANES)),
        select,
        contract,
        precision=lax.Precision.HIGHEST,
        preferred_element_type=jnp.float32,
    )[0:1, :]
    score = -pref_beta * (difference - margins)
    pair_row = jnp.maximum(score, 0.0) + log_one_plus(jnp.exp(-jnp.abs(score)))
    z_row = zloss_weight * row / live
    seq_out[...] = seq_row[:, :seqs]
    pair_out[...] = pair_row[:, :pairs]
    z_out[...] = z_row[:, seqs : seqs + 1]
    drain(other_sums, sums_sem.at[0])


def per_device(dims, hidden, head_weight, labels, lengths, pair_map, ref_margin):
    ny, nx, nz = dims
    plane = ny * nx
    window, width = hidden.shape
    columns = head_weight.shape[1]
    seqs = lengths.shape[0]
    live = seqs * window // 2
    rows = live // nz
    slots = -(-window // (nz * 16)) * 16
    bf16, f32, i32 = jnp.bfloat16, jnp.float32, jnp.int32
    vmem = pltpu.VMEM
    dma = pltpu.SemaphoreType.DMA
    seq_logps, pair_loss, z_loss = pl.pallas_call(
        functools.partial(kernel, dims),
        out_shape=[jax.ShapeDtypeStruct((1, n), f32) for n in (seqs, seqs // 2, 1)],
        in_specs=[
            pl.BlockSpec(memory_space=pl.ANY),
            pl.BlockSpec(memory_space=pl.ANY),
            pl.BlockSpec(memory_space=vmem),
            pl.BlockSpec(memory_space=pltpu.SMEM),
            pl.BlockSpec(memory_space=pltpu.SMEM),
            pl.BlockSpec(memory_space=pltpu.SMEM),
        ],
        out_specs=[pl.BlockSpec(memory_space=vmem)] * 3,
        scratch_shapes=[
            vmem((window, width), bf16),
            vmem((width, columns), bf16),
            vmem((2 * plane, slots, LANES), bf16),
            vmem((2 * plane, slots, LANES), bf16),
            vmem((1, LANES), i32),
            vmem((2 * plane, 1, LANES), i32),
            vmem((2, plane * nz, rows, LANES), bf16),
            vmem((nz, rows, columns), f32),
            vmem((nz, rows, LANES), f32),
            vmem((nz, rows - rows * nz // plane + LANES, LANES), f32),
            vmem((plane, 4, LANES), f32),
            vmem((plane, 4, LANES), f32),
            vmem((4, LANES), f32),
            vmem((2 * nz, 4, LANES), f32),
            vmem((1, LANES), f32),
            vmem((plane, 1, LANES), f32),
            dma((2,)),
            dma((2,)),
            dma((2,)),
            dma(()),
            dma(()),
            dma((CUTS * plane * nz,)),
            dma((plane * nz,)),
            dma((2,)),
            dma((2,)),
            dma((2,)),
        ],
        compiler_params=pltpu.CompilerParams(collective_id=0, has_side_effects=True),
    )(hidden, head_weight, labels.reshape(1, window), lengths, pair_map, ref_margin)
    return seq_logps.reshape(seqs), pair_loss.reshape(seqs // 2), z_loss.reshape(())


def solution(mesh):
    nz = mesh.shape["vocab"]
    ny = nx = {32: 4, 8: 2}[mesh.shape["seq"]]
    torus = Mesh(
        mesh.devices.reshape(ny, nx, 2, nz), ("seq_0", "seq_1", "seq_2", "vocab")
    )
    return jax.shard_map(
        functools.partial(per_device, (ny, nx, nz)),
        mesh=torus,
        in_specs=(P(SEQ, None), P(None, SEQ_VOCAB), P(SEQ), P(), P(), P()),
        out_specs=(P(), P(), P()),
        check_vma=False,
    )
```

```python
import functools
import heapq
import math

import jax
import jax.numpy as jnp
from jax import lax
from jax.experimental import pallas as pl
from jax.experimental.pallas import tpu as pltpu
from jax.sharding import Mesh
from jax.sharding import PartitionSpec as P

SEQ = ("seq_0", "seq_1", "seq_2")
SEQ_VOCAB = ("seq_0", "seq_1", "seq_2", "vocab")
MESH = pl.DeviceIdType.MESH

pref_beta = 0.05
zloss_weight = 0.0001

LANES = 128
CHUNK = 4
CUTS = 2
BACKLOG = 1.8
WIRE = 1.33
HOP = 2.2
TWIN = 1.6
ISSUE = 0.012
PAIR = 0.108
PLACE = 0.35
STATS = 0.35

STEPS = [(0, 1), (0, -1), (1, 1), (1, -1), (2, 1), (2, -1)]
WAYS = [
    4, 4, 4, 5, 5, 5, 5, 2, 2, 4, 4, 4, 2, 2, 2, 3, 4, 2, 3, 5, 2, 3, 5, 3, 4, 3, 3, 3, 5, 3, 3, 0,
    0, 4, 0, 4, 0, 5, 0, 0, 4, 0, 2, 0, 5, 0, 0, 0, 2, 2, 0, 2, 3, 3, 3, 3, 0, 3, 4, 3, 5, 0, 5, 1,
    0, 4, 0, 0, 5, 0, 1, 1, 1, 0, 2, 1, 5, 0, 2, 3, 4, 4, 3, 2, 5, 1, 0, 1, 1, 4, 4, 5, 5, 5, 3, 1,
    1, 4, 1, 5, 1, 1, 5, 2, 4, 1, 1, 2, 2, 1, 2, 2, 1, 2, 2, 2, 1, 5, 1, 1, 1, 3, 4, 4, 3, 5, 3,
]


def broadcast_tree(dims):
    nodes = [
        (a, b, c)
        for a in range(dims[0])
        for b in range(dims[1])
        for c in range(dims[2])
        if (a, b, c) != (0, 0, 0)
    ]
    if len(nodes) == len(WAYS):
        return {node: STEPS[way] for node, way in zip(nodes, WAYS)}
    taken = {}
    for node in nodes:
        axis = next(k for k in range(3) if node[k])
        taken[node] = (axis, 1 if node[axis] <= dims[axis] // 2 else -1)
    return taken


def before(node, way, dims):
    place = list(node)
    place[way[0]] = (place[way[0]] - way[1]) % dims[way[0]]
    return tuple(place)


def gather_plan(dims, cuts):
    taken = broadcast_tree(dims)
    children = {}
    for node, way in taken.items():
        children.setdefault(before(node, way, dims), []).append((node, way))

    @functools.cache
    def height(node):
        return max([1 + height(child) for child, _ in children.get(node, [])], default=0)

    @functools.cache
    def weight(node):
        return 1 + sum(weight(child) for child, _ in children.get(node, []))

    wire = WIRE / cuts
    ways = sorted(set(taken.values()))
    ready = {way: [] for way in ways}
    free = {way: 0.0 for way in ways}
    left = {way: cuts * sum(w == way for w in taken.values()) for way in ways}
    arrivals = [(0.0, cut, ((0, 0, 0), cut)) for cut in range(cuts)]
    count = cuts
    now = 0.0
    plan = []
    arrived = {}
    waiting = {}
    multiplied = 0
    cost = PAIR * CHUNK
    ranks = sorted(range(dims[2]), key=lambda dz: (min(dz, dims[2] - dz), dz))
    places = list(ranks)
    missing = {dz: dims[0] * dims[1] for dz in ranks}
    finished = []

    def multiply(nodes):
        plan.append(("multiply", tuple(nodes), None, None))
        for node in nodes:
            del waiting[node]
            missing[node[2]] -= 1
            if not missing[node[2]]:
                finished.append(node[2])

    def urgency(piece):
        node, cut = piece
        return (-height(node), -weight(node), ranks.index(node[2]), cut, node)

    while arrivals or waiting:
        while arrivals and arrivals[0][0] <= now:
            piece = heapq.heappop(arrivals)[2]
            node, cut = piece
            plan.append(("wait", piece, None, None))
            now += ISSUE
            for child, way in children.get(node, []):
                ready[way].append((child, cut))
            arrived[node] = arrived.get(node, 0) + 1
            if arrived[node] == cuts:
                plan.append(("twin", node, None, None))
                now += ISSUE
                waiting[node] = now + TWIN
        for way in ways:
            while ready[way] and free[way] - now < BACKLOG - 0.5 * wire:
                ready[way].sort(key=urgency)
                piece = ready[way].pop(0)
                free[way] = max(now, free[way]) + wire
                left[way] -= 1
                plan.append(("send", (before(piece[0], way, dims), piece[1]), piece, way))
                now += ISSUE
                heapq.heappush(arrivals, (free[way] + HOP, count, piece))
                count += 1
        if arrivals and arrivals[0][0] <= now:
            continue
        coming = arrivals[0][0] if arrivals else math.inf
        queued = min([free[way] - now for way in ways if left[way]], default=math.inf)
        there = [node for node, when in waiting.items() if when <= now]
        there.sort(key=lambda node: ranks.index(node[2]))
        if finished and finished[0] not in places:
            if queued >= STATS or coming >= now + STATS:
                plan.append(("stats", finished.pop(0), None, None))
                now += STATS
                continue
        if len(there) >= CHUNK and (queued >= cost or coming >= now + cost or len(waiting) > 32):
            multiply(there[:CHUNK])
            multiplied += CHUNK
            now += cost
            continue
        if places and multiplied >= 2 * CHUNK:
            if queued >= PLACE or coming >= now + PLACE:
                plan.append(("place", places.pop(0), None, None))
                now += PLACE
                continue
        later = [coming]
        later += [free[way] - BACKLOG + 0.5 * wire for way in ways if ready[way]]
        if len(waiting) >= CHUNK:
            later.append(max(sorted(waiting.values())[CHUNK - 1], now + 0.05))
        if min(later) == math.inf:
            multiply(list(waiting)[:CHUNK])
            now += cost
            continue
        now = max(now + 1e-6, min(later))
    for dz in places:
        plan.append(("place", dz, None, None))
    for dz in finished:
        plan.append(("stats", dz, None, None))
    return plan


def log_one_plus(u):
    w = u / (2.0 + u)
    square = w * w
    total = jnp.full_like(w, 1.0 / 17.0)
    for odd in (15, 13, 11, 9, 7, 5, 3, 1):
        total = total * square + 1.0 / odd
    return 2.0 * w * total


def iota(shape, dim):
    return lax.broadcasted_iota(jnp.int32, shape, dim)


def scatter_scalars(ids, values):
    out = jnp.zeros(ids.shape, jnp.int32)
    for k, value in enumerate(values):
        out = jnp.where(ids == k, value, out)
    return out


def sums_before(ids, values):
    out = jnp.zeros(ids.shape, jnp.int32)
    for k, value in enumerate(values):
        out = out + jnp.where(ids > k, value, 0)
    return out


def kernel(
    dims,
    hidden_hbm,
    weight_hbm,
    labels_ref,
    lengths_ref,
    pairs_ref,
    margins_ref,
    seq_out,
    pair_out,
    z_out,
    hidden,
    weight,
    parcels,
    received,
    label_row,
    labels_all,
    gathered,
    scores,
    label_place,
    packed,
    stats,
    stats_in,
    merged,
    merged_in,
    sums,
    sums_in,
    load_sem,
    parcel_sem,
    label_sem,
    block_send,
    twin_send,
    block_recv,
    twin_recv,
    stat_sem,
    merged_sem,
    sums_sem,
):
    ny, nx, nz = dims
    plane = ny * nx
    seqs = lengths_ref.shape[0]
    pairs = margins_ref.shape[0]
    window = hidden.shape[0]
    slots = parcels.shape[1]
    rows = gathered.shape[2]
    columns = weight.shape[1]
    halves = plane // nz
    part_rows = rows // halves
    y, x = lax.axis_index("seq_0"), lax.axis_index("seq_1")
    core, z = lax.axis_index("seq_2"), lax.axis_index("vocab")
    here = y * nx + x
    mine = here * 2 + core
    twin = 1 - core

    def shifted(dy, dx, dz):
        return ((y + dy) % ny, (x + dx) % nx, (z + dz) % nz)

    def chip_of(node):
        cy, cx, cz = shifted(-node[0] + ny, -node[1] + nx, -node[2] + nz)
        return (cy * nx + cx) * nz + cz

    load_hidden = pltpu.make_async_copy(hidden_hbm, hidden, load_sem.at[0])
    load_weight = pltpu.make_async_copy(weight_hbm, weight, load_sem.at[1])
    load_hidden.start()

    far = lambda n, size: min(n, size - n)
    plane_steps = sorted(
        [(a, b) for a in range(ny) for b in range(nx)],
        key=lambda s: -(far(s[0], ny) + far(s[1], nx)),
    )
    plane_peers = [(a, b, c) for a, b in plane_steps for c in (0, 1) if (a, b, c) != (0, 0, 0)]

    def peer_of(step):
        py, px, _ = shifted(step[0], step[1], 0)
        pc = twin if step[2] else core
        return py, px, pc

    barrier = pltpu.get_barrier_semaphore()
    for step in plane_peers:
        py, px, pc = peer_of(step)
        pl.semaphore_signal(barrier, inc=1, device_id=(py, px, pc, z), device_id_type=MESH)
    z_steps = sorted({1 % nz, nz - 1} - {0})
    for dz in z_steps:
        pl.semaphore_signal(
            barrier, inc=1, device_id=(y, x, core, (z + dz) % nz), device_id_type=MESH
        )

    lens = [lengths_ref[s] for s in range(seqs)]
    own_first = jnp.int32(0)
    for s in range(seqs - 1):
        own_first = own_first + jnp.where(mine > s, lens[s], 0)
    own_place = nz * iota((slots, window), 0) + ((z - own_first) & (nz - 1))
    choose = jnp.where(own_place == iota((slots, window), 1), 1.0, 0.0).astype(jnp.bfloat16)

    label_row[...] = jnp.zeros(label_row.shape, jnp.int32)
    label_row[0:1, 0:window] = labels_ref[...]
    labels_all[mine] = label_row[...]
    load_hidden.wait()
    load_weight.start()
    chosen = jnp.dot(choose, hidden[...], preferred_element_type=jnp.float32)
    chosen = chosen.astype(jnp.bfloat16)
    for j in range(2 * plane):
        parcels[j] = chosen[:, j * LANES : (j + 1) * LANES]
    received[mine] = parcels[mine]

    pl.semaphore_wait(barrier, len(plane_peers) + len(z_steps))

    for step in plane_peers:
        py, px, pc = peer_of(step)
        pltpu.make_async_remote_copy(
            src_ref=parcels.at[(py * nx + px) * 2 + pc],
            dst_ref=received.at[mine],
            send_sem=parcel_sem.at[0],
            recv_sem=parcel_sem.at[1],
            device_id=(py, px, pc, z),
            device_id_type=MESH,
        ).start()
    for step in plane_peers:
        py, px, pc = peer_of(step)
        pltpu.make_async_remote_copy(
            src_ref=label_row,
            dst_ref=labels_all.at[mine],
            send_sem=label_sem.at[0],
            recv_sem=label_sem.at[1],
            device_id=(py, px, pc, z),
            device_id_type=MESH,
        ).start()
    slot_ids = iota((1, seqs * slots), 1)
    slot_seq = slot_ids // slots
    first = sums_before(slot_seq, lens)
    place = nz * (slot_ids % slots) + ((z - first) & (nz - 1))
    row_of_slot = jnp.where(
        place < scatter_scalars(slot_seq, lens), (first + place - z) // nz, -1
    )
    scores[...] = jnp.zeros(scores.shape, jnp.float32)
    compact = jnp.where(iota((rows, seqs * slots), 0) == row_of_slot, 1.0, 0.0)
    compact = compact.astype(jnp.bfloat16)
    others = received.at[pl.ds(0, 2 * plane - 1)]
    pltpu.make_async_copy(others, others, parcel_sem.at[1]).wait()
    block = jnp.dot(
        compact,
        received[...].reshape(seqs * slots, LANES),
        preferred_element_type=jnp.float32,
    )
    own_chip = here * nz + z
    gathered[core, own_chip] = block.astype(jnp.bfloat16)

    lane = iota((1, LANES), 1)
    lane_first = sums_before(lane, lens)
    lane_len = scatter_scalars(lane, lens)
    sub = iota((LANES, LANES), 0)
    sub_first = sums_before(sub, lens)
    sub_len = scatter_scalars(sub, lens)

    def label_table():
        row_ids = iota((LANES, LANES), 0)
        table = jnp.zeros((LANES, LANES), jnp.int32)
        for s in range(seqs):
            table = jnp.where(row_ids == s, labels_all[s], table)
        col_first = (mine * nz + z) * columns
        local = table - col_first
        code = jnp.where((local >= 0) & (local < columns), local + 1, 0)
        pieces = [code // 16, code % 16, sub_first // 16, sub_first % 16]
        return [piece.astype(jnp.float32).astype(jnp.bfloat16) for piece in pieces]

    def place_labels(pieces, zz):
        ids = nz * iota((rows, LANES), 0) + zz
        member = (ids >= lane_first) & (ids < lane_first + lane_len)
        member = jnp.where(member, 1.0, 0.0).astype(jnp.bfloat16)
        high, low, first_high, first_low = [
            jnp.dot(member, piece, preferred_element_type=jnp.float32) for piece in pieces
        ]
        position = ids.astype(jnp.float32) - (16.0 * first_high + first_low)
        at = position == iota((rows, LANES), 1).astype(jnp.float32)
        code = jnp.sum(jnp.where(at, 16.0 * high + low, 0.0), axis=1, keepdims=True)
        label_place[zz] = jnp.broadcast_to(code - 1.0, (rows, LANES))

    def multiply(chips):
        products = []
        for chip in chips:
            depth = pl.multiple_of((chip // nz) * (2 * LANES), 2 * LANES)
            pair = jnp.concatenate([gathered[0, chip], gathered[1, chip]], axis=1)
            product = jnp.dot(
                pair, weight[pl.ds(depth, 2 * LANES), :], preferred_element_type=jnp.float32
            )
            products.append((chip % nz, product))
        for zz, product in products:
            scores[zz] = scores[zz] + product

    spot = iota((rows, LANES), 1)

    def summarize(zz):
        tiles = [scores[zz, :, k : k + LANES] for k in range(0, columns, LANES)]
        top = jnp.max(functools.reduce(jnp.maximum, tiles), axis=1, keepdims=True)
        total = functools.reduce(jnp.add, [jnp.exp(tile - top) for tile in tiles])
        total = jnp.sum(total, axis=1, keepdims=True)
        code = label_place[zz]
        picked = functools.reduce(
            jnp.add,
            [
                jnp.where(code - float(k * LANES) == spot.astype(jnp.float32), tile, 0.0)
                for k, tile in enumerate(tiles)
            ],
        )
        picked = jnp.sum(picked, axis=1, keepdims=True)
        packed[0:rows, :] = jnp.where(spot == 0, top, jnp.where(spot == 1, total, picked))
        for half in range(halves):
            j = zz * halves + half
            start = half * part_rows
            stats[j] = packed[start : start + LANES, :].T[0:4, :]

            @pl.when(j != here)
            def _():
                pltpu.make_async_remote_copy(
                    src_ref=stats.at[j],
                    dst_ref=stats_in.at[here],
                    send_sem=stat_sem.at[0],
                    recv_sem=stat_sem.at[1],
                    device_id=(j // nx, j % nx, core, z),
                    device_id_type=MESH,
                ).start()

    packed[rows:, :] = jnp.zeros((LANES - part_rows, LANES), jnp.float32)
    edges = [0, LANES, rows] if CUTS == 2 else [0, rows]
    plan = gather_plan(dims, CUTS)
    order = {}
    for kind, item, _, _ in plan:
        if kind == "twin":
            order[item] = len(order)

    def piece_ref(node, cut):
        return gathered.at[core, chip_of(node), pl.ds(edges[cut], edges[cut + 1] - edges[cut])]

    def drain(ref, sem):
        pltpu.make_async_copy(ref, ref, sem).wait()

    pieces = None
    first_product = True
    for kind, item, child, way in plan:
        if kind == "wait":
            node, cut = item
            if node != (0, 0, 0):
                drain(piece_ref(node, cut), block_recv.at[order[node] * CUTS + cut])
        elif kind == "twin":
            ref = gathered.at[core, chip_of(item)]
            pltpu.make_async_remote_copy(
                src_ref=ref,
                dst_ref=ref,
                send_sem=twin_send,
                recv_sem=twin_recv.at[order[item]],
                device_id=(y, x, twin, z),
                device_id_type=MESH,
            ).start()
        elif kind == "send":
            node, cut = item
            ref = piece_ref(node, cut)
            step = [0, 0, 0]
            step[way[0]] = way[1] % dims[way[0]]
            ty, tx, tz = shifted(*step)
            pltpu.make_async_remote_copy(
                src_ref=ref,
                dst_ref=ref,
                send_sem=block_send,
                recv_sem=block_recv.at[order[child[0]] * CUTS + cut],
                device_id=(ty, tx, core, tz),
                device_id_type=MESH,
            ).start()
        elif kind == "multiply":
            if first_product:
                load_weight.wait()
                first_product = False
            for node in item:
                drain(gathered.at[twin, chip_of(node)], twin_recv.at[order[node]])
            multiply([chip_of(node) for node in item])
        elif kind == "stats":
            summarize((z + nz - item) % nz)
        else:
            if pieces is None:
                drain(labels_all.at[pl.ds(0, 2 * plane - 1)], label_sem.at[1])
                pieces = label_table()
            place_labels(pieces, (z + nz - item) % nz)

    plane_chips = [s for s in plane_steps if s != (0, 0)]
    stats_in[here] = stats[here]
    other_stats = stats_in.at[pl.ds(0, plane - 1)]
    pltpu.make_async_copy(other_stats, other_stats, stat_sem.at[1]).wait()

    def merge(ref, count):
        tops = [ref[k, 0:1, :] for k in range(count)]
        top = functools.reduce(jnp.maximum, tops)
        total = functools.reduce(
            jnp.add, [ref[k, 1:2, :] * jnp.exp(tops[k] - top) for k in range(count)]
        )
        picked = functools.reduce(jnp.add, [ref[k, 2:3, :] for k in range(count)])
        return top, total, picked

    top, total, picked = merge(stats_in, plane)
    merged[0:1, :] = top
    merged[1:2, :] = total
    merged[2:3, :] = picked
    merged[3:4, :] = jnp.zeros((1, LANES), jnp.float32)
    line = z * 2 + core
    merged_in[line] = merged[...]
    line_peers = sorted(
        [(dz, dc) for dz in range(nz) for dc in (0, 1) if (dz, dc) != (0, 0)],
        key=lambda s: -far(s[0], nz),
    )
    for dz, dc in line_peers:
        pltpu.make_async_remote_copy(
            src_ref=merged,
            dst_ref=merged_in.at[line],
            send_sem=merged_sem.at[0],
            recv_sem=merged_sem.at[1],
            device_id=(y, x, twin if dc else core, (z + dz) % nz),
            device_id_type=MESH,
        ).start()
    other_merged = merged_in.at[pl.ds(0, 2 * nz - 1)]
    pltpu.make_async_copy(other_merged, other_merged, merged_sem.at[1]).wait()

    top, total, picked = merge(merged_in, 2 * nz)
    filled = lane < part_rows
    log_norm = top + jnp.log(jnp.where(filled, total, 1.0))
    gain = jnp.where(filled, picked - log_norm, 0.0)
    row_ids = nz * ((here % halves) * part_rows + lane) + here // halves
    inside = (row_ids >= sub_first) & (row_ids < sub_first + sub_len)
    inside = jnp.where(inside, 1.0, 0.0)
    contract = (((1,), (1,)), ((), ()))
    by_seq = lax.dot_general(
        jnp.broadcast_to(gain, (8, LANES)),
        inside,
        contract,
        precision=lax.Precision.HIGHEST,
        preferred_element_type=jnp.float32,
    )[0:1, :]
    squares = jnp.sum(jnp.where(filled, log_norm * log_norm, 0.0), axis=1, keepdims=True)
    sums[...] = jnp.where(lane == seqs, squares, by_seq)
    sums_in[here] = sums[...]
    for a, b in plane_chips:
        py, px, _ = shifted(a, b, 0)
        pltpu.make_async_remote_copy(
            src_ref=sums,
            dst_ref=sums_in.at[here],
            send_sem=sums_sem.at[0],
            recv_sem=sums_sem.at[1],
            device_id=(py, px, core, z),
            device_id_type=MESH,
        ).start()
    pair_ids = iota((LANES, LANES), 0)
    select = jnp.zeros((LANES, LANES), jnp.float32)
    seq_ids = iota((LANES, LANES), 1)
    margins = jnp.zeros((1, LANES), jnp.float32)
    for p in range(pairs):
        hit = jnp.where(seq_ids == pairs_ref[2 * p], 1.0, 0.0)
        hit = hit - jnp.where(seq_ids == pairs_ref[2 * p + 1], 1.0, 0.0)
        select = jnp.where(pair_ids == p, hit, select)
        margins = jnp.where(lane == p, margins_ref[p], margins)
    live = functools.reduce(jnp.add, lens).astype(jnp.float32)

    drain(others, parcel_sem.at[0])
    drain(labels_all.at[pl.ds(0, 2 * plane - 1)], label_sem.at[0])
    drain(gathered.at[0, pl.ds(0, plane * nz - 1)], block_send)
    drain(gathered.at[0], twin_send)
    drain(other_stats, stat_sem.at[0])
    drain(other_merged, merged_sem.at[0])
    other_sums = sums_in.at[pl.ds(0, plane - 1)]
    drain(other_sums, sums_sem.at[1])

    row = functools.reduce(jnp.add, [sums_in[k] for k in range(plane)])
    seq_row = jnp.where(lane < seqs, row, 0.0)
    difference = lax.dot_general(
        jnp.broadcast_to(seq_row, (8, LANES)),
        select,
        contract,
        precision=lax.Precision.HIGHEST,
        preferred_element_type=jnp.float32,
    )[0:1, :]
    score = -pref_beta * (difference - margins)
    pair_row = jnp.maximum(score, 0.0) + log_one_plus(jnp.exp(-jnp.abs(score)))
    z_row = zloss_weight * row / live
    seq_out[...] = seq_row[:, :seqs]
    pair_out[...] = pair_row[:, :pairs]
    z_out[...] = z_row[:, seqs : seqs + 1]
    drain(other_sums, sums_sem.at[0])


def per_device(dims, hidden, head_weight, labels, lengths, pair_map, ref_margin):
    ny, nx, nz = dims
    plane = ny * nx
    window, width = hidden.shape
    columns = head_weight.shape[1]
    seqs = lengths.shape[0]
    live = seqs * window // 2
    rows = live // nz
    slots = -(-window // (nz * 16)) * 16
    bf16, f32, i32 = jnp.bfloat16, jnp.float32, jnp.int32
    vmem = pltpu.VMEM
    dma = pltpu.SemaphoreType.DMA
    seq_logps, pair_loss, z_loss = pl.pallas_call(
        functools.partial(kernel, dims),
        out_shape=[jax.ShapeDtypeStruct((1, n), f32) for n in (seqs, seqs // 2, 1)],
        in_specs=[
            pl.BlockSpec(memory_space=pl.ANY),
            pl.BlockSpec(memory_space=pl.ANY),
            pl.BlockSpec(memory_space=vmem),
            pl.BlockSpec(memory_space=pltpu.SMEM),
            pl.BlockSpec(memory_space=pltpu.SMEM),
            pl.BlockSpec(memory_space=pltpu.SMEM),
        ],
        out_specs=[pl.BlockSpec(memory_space=vmem)] * 3,
        scratch_shapes=[
            vmem((window, width), bf16),
            vmem((width, columns), bf16),
            vmem((2 * plane, slots, LANES), bf16),
            vmem((2 * plane, slots, LANES), bf16),
            vmem((1, LANES), i32),
            vmem((2 * plane, 1, LANES), i32),
            vmem((2, plane * nz, rows, LANES), bf16),
            vmem((nz, rows, columns), f32),
            vmem((nz, rows, LANES), f32),
            vmem((rows - rows * nz // plane + LANES, LANES), f32),
            vmem((plane, 4, LANES), f32),
            vmem((plane, 4, LANES), f32),
            vmem((4, LANES), f32),
            vmem((2 * nz, 4, LANES), f32),
            vmem((1, LANES), f32),
            vmem((plane, 1, LANES), f32),
            dma((2,)),
            dma((2,)),
            dma((2,)),
            dma(()),
            dma(()),
            dma((CUTS * plane * nz,)),
            dma((plane * nz,)),
            dma((2,)),
            dma((2,)),
            dma((2,)),
        ],
        compiler_params=pltpu.CompilerParams(collective_id=0, has_side_effects=True),
    )(hidden, head_weight, labels.reshape(1, window), lengths, pair_map, ref_margin)
    return seq_logps.reshape(seqs), pair_loss.reshape(seqs // 2), z_loss.reshape(())


def solution(mesh):
    nz = mesh.shape["vocab"]
    ny = nx = {32: 4, 8: 2}[mesh.shape["seq"]]
    torus = Mesh(
        mesh.devices.reshape(ny, nx, 2, nz), ("seq_0", "seq_1", "seq_2", "vocab")
    )
    return jax.shard_map(
        functools.partial(per_device, (ny, nx, nz)),
        mesh=torus,
        in_specs=(P(SEQ, None), P(None, SEQ_VOCAB), P(SEQ), P(), P(), P()),
        out_specs=(P(), P(), P()),
        check_vma=False,
    )
```

```python
import functools
import heapq
import math

import jax
import jax.numpy as jnp
from jax import lax
from jax.experimental import pallas as pl
from jax.experimental.pallas import tpu as pltpu
from jax.sharding import Mesh
from jax.sharding import PartitionSpec as P

SEQ = ("seq_0", "seq_1", "seq_2")
SEQ_VOCAB = ("seq_0", "seq_1", "seq_2", "vocab")
MESH = pl.DeviceIdType.MESH

pref_beta = 0.05
zloss_weight = 0.0001

LANES = 128
CHUNK = 4
CUTS = 2
BACKLOG = 1.8
WIRE = 1.33
HOP = 2.2
TWIN = 1.6
ISSUE = 0.012
PAIR = 0.108
PLACE = 0.35
STATS = 0.35

STEPS = [(0, 1), (0, -1), (1, 1), (1, -1), (2, 1), (2, -1)]
WAYS = [
    4, 4, 4, 5, 5, 5, 5, 2, 2, 4, 4, 4, 2, 2, 2, 3, 4, 2, 3, 5, 2, 3, 5, 3, 4, 3, 3, 3, 5, 3, 3, 0,
    0, 4, 0, 4, 0, 5, 0, 0, 4, 0, 2, 0, 5, 0, 0, 0, 2, 2, 0, 2, 3, 3, 3, 3, 0, 3, 4, 3, 5, 0, 5, 1,
    0, 4, 0, 0, 5, 0, 1, 1, 1, 0, 2, 1, 5, 0, 2, 3, 4, 4, 3, 2, 5, 1, 0, 1, 1, 4, 4, 5, 5, 5, 3, 1,
    1, 4, 1, 5, 1, 1, 5, 2, 4, 1, 1, 2, 2, 1, 2, 2, 1, 2, 2, 2, 1, 5, 1, 1, 1, 3, 4, 4, 3, 5, 3,
]


def broadcast_tree(dims):
    nodes = [
        (a, b, c)
        for a in range(dims[0])
        for b in range(dims[1])
        for c in range(dims[2])
        if (a, b, c) != (0, 0, 0)
    ]
    if len(nodes) == len(WAYS):
        return {node: STEPS[way] for node, way in zip(nodes, WAYS)}
    taken = {}
    for node in nodes:
        axis = next(k for k in range(3) if node[k])
        taken[node] = (axis, 1 if node[axis] <= dims[axis] // 2 else -1)
    return taken


def before(node, way, dims):
    place = list(node)
    place[way[0]] = (place[way[0]] - way[1]) % dims[way[0]]
    return tuple(place)


def gather_plan(dims, cuts):
    taken = broadcast_tree(dims)
    children = {}
    for node, way in taken.items():
        children.setdefault(before(node, way, dims), []).append((node, way))

    @functools.cache
    def height(node):
        return max([1 + height(child) for child, _ in children.get(node, [])], default=0)

    @functools.cache
    def weight(node):
        return 1 + sum(weight(child) for child, _ in children.get(node, []))

    wire = WIRE / cuts
    ways = sorted(set(taken.values()))
    ready = {way: [] for way in ways}
    free = {way: 0.0 for way in ways}
    left = {way: cuts * sum(w == way for w in taken.values()) for way in ways}
    arrivals = [(0.0, cut, ((0, 0, 0), cut)) for cut in range(cuts)]
    count = cuts
    now = 0.0
    plan = []
    arrived = {}
    waiting = {}
    multiplied = 0
    cost = PAIR * CHUNK
    ranks = sorted(range(dims[2]), key=lambda dz: (min(dz, dims[2] - dz), dz))
    places = list(ranks)
    missing = {dz: dims[0] * dims[1] for dz in ranks}
    finished = []

    def multiply(nodes):
        plan.append(("multiply", tuple(nodes), None, None))
        for node in nodes:
            del waiting[node]
            missing[node[2]] -= 1
            if not missing[node[2]]:
                finished.append(node[2])

    def urgency(piece):
        node, cut = piece
        return (-height(node), -weight(node), ranks.index(node[2]), cut, node)

    while arrivals or waiting:
        while arrivals and arrivals[0][0] <= now:
            piece = heapq.heappop(arrivals)[2]
            node, cut = piece
            plan.append(("wait", piece, None, None))
            now += ISSUE
            for child, way in children.get(node, []):
                ready[way].append((child, cut))
            arrived[node] = arrived.get(node, 0) + 1
            if arrived[node] == cuts:
                plan.append(("twin", node, None, None))
                now += ISSUE
                waiting[node] = now + TWIN
        for way in ways:
            while ready[way] and free[way] - now < BACKLOG - 0.5 * wire:
                ready[way].sort(key=urgency)
                piece = ready[way].pop(0)
                free[way] = max(now, free[way]) + wire
                left[way] -= 1
                plan.append(("send", (before(piece[0], way, dims), piece[1]), piece, way))
                now += ISSUE
                heapq.heappush(arrivals, (free[way] + HOP, count, piece))
                count += 1
        if arrivals and arrivals[0][0] <= now:
            continue
        coming = arrivals[0][0] if arrivals else math.inf
        queued = min([free[way] - now for way in ways if left[way]], default=math.inf)
        there = [node for node, when in waiting.items() if when <= now]
        there.sort(key=lambda node: ranks.index(node[2]))
        if finished and finished[0] not in places:
            if queued >= STATS or coming >= now + STATS:
                plan.append(("stats", finished.pop(0), None, None))
                now += STATS
                continue
        if len(there) >= CHUNK and (queued >= cost or coming >= now + cost or len(waiting) > 32):
            multiply(there[:CHUNK])
            multiplied += CHUNK
            now += cost
            continue
        if places and multiplied >= 2 * CHUNK:
            if queued >= PLACE or coming >= now + PLACE:
                plan.append(("place", places.pop(0), None, None))
                now += PLACE
                continue
        later = [coming]
        later += [free[way] - BACKLOG + 0.5 * wire for way in ways if ready[way]]
        if len(waiting) >= CHUNK:
            later.append(max(sorted(waiting.values())[CHUNK - 1], now + 0.05))
        if min(later) == math.inf:
            multiply(list(waiting)[:CHUNK])
            now += cost
            continue
        now = max(now + 1e-6, min(later))
    for dz in places:
        plan.append(("place", dz, None, None))
    for dz in finished:
        plan.append(("stats", dz, None, None))
    return plan


def log_one_plus(u):
    w = u / (2.0 + u)
    square = w * w
    total = jnp.full_like(w, 1.0 / 17.0)
    for odd in (15, 13, 11, 9, 7, 5, 3, 1):
        total = total * square + 1.0 / odd
    return 2.0 * w * total


def iota(shape, dim):
    return lax.broadcasted_iota(jnp.int32, shape, dim)


def scatter_scalars(ids, values):
    out = jnp.zeros(ids.shape, jnp.int32)
    for k, value in enumerate(values):
        out = jnp.where(ids == k, value, out)
    return out


def sums_before(ids, values):
    out = jnp.zeros(ids.shape, jnp.int32)
    for k, value in enumerate(values):
        out = out + jnp.where(ids > k, value, 0)
    return out


def kernel(
    dims,
    hidden_hbm,
    weight_hbm,
    labels_ref,
    lengths_ref,
    pairs_ref,
    margins_ref,
    out_ref,
    hidden,
    weight,
    parcels,
    received,
    label_row,
    labels_all,
    gathered,
    scores,
    label_place,
    packed,
    stats,
    stats_in,
    merged,
    merged_in,
    sums,
    sums_in,
    load_sem,
    parcel_sem,
    label_sem,
    block_send,
    twin_send,
    block_recv,
    twin_recv,
    stat_sem,
    merged_sem,
    sums_sem,
):
    ny, nx, nz = dims
    plane = ny * nx
    seqs = lengths_ref.shape[0]
    pairs = margins_ref.shape[0]
    window = hidden.shape[0]
    slots = parcels.shape[1]
    rows = gathered.shape[2]
    columns = weight.shape[1]
    part_rows = 15 * LANES // 16
    parts = rows // part_rows
    pack = nz // nx
    owners = 2 * nx
    y, x = lax.axis_index("seq_0"), lax.axis_index("seq_1")
    core, z = lax.axis_index("seq_2"), lax.axis_index("vocab")
    here = y * nx + x
    mine = here * 2 + core
    twin = 1 - core
    rank = x * 2 + core

    def shifted(dy, dx, dz):
        return ((y + dy) % ny, (x + dx) % nx, (z + dz) % nz)

    def chip_of(node):
        cy, cx, cz = shifted(-node[0] + ny, -node[1] + nx, -node[2] + nz)
        return (cy * nx + cx) * nz + cz

    load_hidden = pltpu.make_async_copy(hidden_hbm, hidden, load_sem.at[0])
    load_weight = pltpu.make_async_copy(weight_hbm, weight, load_sem.at[1])
    load_hidden.start()

    far = lambda n, size: min(n, size - n)
    plane_steps = sorted(
        [(a, b) for a in range(ny) for b in range(nx)],
        key=lambda s: -(far(s[0], ny) + far(s[1], nx)),
    )
    plane_peers = [(a, b, c) for a, b in plane_steps for c in (0, 1) if (a, b, c) != (0, 0, 0)]

    def peer_of(step):
        py, px, _ = shifted(step[0], step[1], 0)
        pc = twin if step[2] else core
        return py, px, pc

    barrier = pltpu.get_barrier_semaphore()
    for step in plane_peers:
        py, px, pc = peer_of(step)
        pl.semaphore_signal(barrier, inc=1, device_id=(py, px, pc, z), device_id_type=MESH)
    z_steps = sorted({1 % nz, nz - 1} - {0})
    for dz in z_steps:
        pl.semaphore_signal(
            barrier, inc=1, device_id=(y, x, core, (z + dz) % nz), device_id_type=MESH
        )

    lens = [lengths_ref[s] for s in range(seqs)]
    own_first = jnp.int32(0)
    for s in range(seqs - 1):
        own_first = own_first + jnp.where(mine > s, lens[s], 0)
    own_place = nz * iota((slots, window), 0) + ((z - own_first) & (nz - 1))
    choose = jnp.where(own_place == iota((slots, window), 1), 1.0, 0.0).astype(jnp.bfloat16)

    label_row[...] = jnp.zeros(label_row.shape, jnp.int32)
    label_row[0:1, 0:window] = labels_ref[...]
    labels_all[mine] = label_row[...]
    load_hidden.wait()
    load_weight.start()
    chosen = jnp.dot(choose, hidden[...], preferred_element_type=jnp.float32)
    chosen = chosen.astype(jnp.bfloat16)
    for j in range(2 * plane):
        parcels[j] = chosen[:, j * LANES : (j + 1) * LANES]
    received[mine] = parcels[mine]

    pl.semaphore_wait(barrier, len(plane_peers) + len(z_steps))

    for step in plane_peers:
        py, px, pc = peer_of(step)
        pltpu.make_async_remote_copy(
            src_ref=parcels.at[(py * nx + px) * 2 + pc],
            dst_ref=received.at[mine],
            send_sem=parcel_sem.at[0],
            recv_sem=parcel_sem.at[1],
            device_id=(py, px, pc, z),
            device_id_type=MESH,
        ).start()
    for step in plane_peers:
        py, px, pc = peer_of(step)
        pltpu.make_async_remote_copy(
            src_ref=label_row,
            dst_ref=labels_all.at[mine],
            send_sem=label_sem.at[0],
            recv_sem=label_sem.at[1],
            device_id=(py, px, pc, z),
            device_id_type=MESH,
        ).start()
    slot_ids = iota((1, seqs * slots), 1)
    slot_seq = slot_ids // slots
    first = sums_before(slot_seq, lens)
    place = nz * (slot_ids % slots) + ((z - first) & (nz - 1))
    row_of_slot = jnp.where(
        place < scatter_scalars(slot_seq, lens), (first + place - z) // nz, -1
    )
    scores[...] = jnp.zeros(scores.shape, jnp.float32)
    compact = jnp.where(iota((rows, seqs * slots), 0) == row_of_slot, 1.0, 0.0)
    compact = compact.astype(jnp.bfloat16)
    others = received.at[pl.ds(0, 2 * plane - 1)]
    pltpu.make_async_copy(others, others, parcel_sem.at[1]).wait()
    block = jnp.dot(
        compact,
        received[...].reshape(seqs * slots, LANES),
        preferred_element_type=jnp.float32,
    )
    own_chip = here * nz + z
    gathered[core, own_chip] = block.astype(jnp.bfloat16)

    lane = iota((1, LANES), 1)
    lane_first = sums_before(lane, lens)
    lane_len = scatter_scalars(lane, lens)
    sub = iota((LANES, LANES), 0)
    sub_first = sums_before(sub, lens)
    sub_len = scatter_scalars(sub, lens)

    def label_table():
        row_ids = iota((LANES, LANES), 0)
        table = jnp.zeros((LANES, LANES), jnp.int32)
        for s in range(seqs):
            table = jnp.where(row_ids == s, labels_all[s], table)
        col_first = (mine * nz + z) * columns
        local = table - col_first
        code = jnp.where((local >= 0) & (local < columns), local + 1, 0)
        pieces = [code // 16, code % 16, sub_first // 16, sub_first % 16]
        return [piece.astype(jnp.float32).astype(jnp.bfloat16) for piece in pieces]

    def place_labels(pieces, zz):
        ids = nz * iota((rows, LANES), 0) + zz
        member = (ids >= lane_first) & (ids < lane_first + lane_len)
        member = jnp.where(member, 1.0, 0.0).astype(jnp.bfloat16)
        high, low, first_high, first_low = [
            jnp.dot(member, piece, preferred_element_type=jnp.float32) for piece in pieces
        ]
        position = ids.astype(jnp.float32) - (16.0 * first_high + first_low)
        at = position == iota((rows, LANES), 1).astype(jnp.float32)
        code = jnp.sum(jnp.where(at, 16.0 * high + low, 0.0), axis=1, keepdims=True)
        label_place[zz] = jnp.broadcast_to(code - 1.0, (rows, LANES))

    def multiply(chips):
        products = []
        for chip in chips:
            depth = pl.multiple_of((chip // nz) * (2 * LANES), 2 * LANES)
            pair = jnp.concatenate([gathered[0, chip], gathered[1, chip]], axis=1)
            product = jnp.dot(
                pair, weight[pl.ds(depth, 2 * LANES), :], preferred_element_type=jnp.float32
            )
            products.append((chip % nz, product))
        for zz, product in products:
            scores[zz] = scores[zz] + product

    spot = iota((rows, LANES), 1)

    def summarize(zz):
        tiles = [scores[zz, :, k : k + LANES] for k in range(0, columns, LANES)]
        top = jnp.max(functools.reduce(jnp.maximum, tiles), axis=1, keepdims=True)
        total = functools.reduce(jnp.add, [jnp.exp(tile - top) for tile in tiles])
        total = jnp.sum(total, axis=1, keepdims=True)
        code = label_place[zz]
        picked = functools.reduce(
            jnp.add,
            [
                jnp.where(code - float(k * LANES) == spot.astype(jnp.float32), tile, 0.0)
                for k, tile in enumerate(tiles)
            ],
        )
        picked = jnp.sum(picked, axis=1, keepdims=True)
        packed[0:rows, :] = jnp.where(spot == 0, top + jnp.log(total), picked)
        for part in range(parts):
            flat = packed[part * part_rows : part * part_rows + LANES, :].T
            slot = part % pack
            owner = zz * (parts // pack) + part // pack
            stats[owner, slot : slot + 1, :] = flat[0:1, :]
            stats[owner, pack + slot : pack + slot + 1, :] = flat[1:2, :]
            if slot == pack - 1:

                @pl.when(owner != rank)
                def _():
                    pltpu.make_async_remote_copy(
                        src_ref=stats.at[owner],
                        dst_ref=stats_in.at[rank],
                        send_sem=stat_sem.at[0],
                        recv_sem=stat_sem.at[1],
                        device_id=(y, owner // 2, owner % 2, z),
                        device_id_type=MESH,
                    ).start()

    packed[rows:, :] = jnp.zeros((LANES - part_rows, LANES), jnp.float32)
    edges = [0, LANES, rows] if CUTS == 2 else [0, rows]
    plan = gather_plan(dims, CUTS)
    order = {}
    for kind, item, _, _ in plan:
        if kind == "twin":
            order[item] = len(order)

    def piece_ref(node, cut):
        return gathered.at[core, chip_of(node), pl.ds(edges[cut], edges[cut + 1] - edges[cut])]

    def drain(ref, sem):
        pltpu.make_async_copy(ref, ref, sem).wait()

    pieces = None
    first_product = True
    for kind, item, child, way in plan:
        if kind == "wait":
            node, cut = item
            if node != (0, 0, 0):
                drain(piece_ref(node, cut), block_recv.at[order[node] * CUTS + cut])
        elif kind == "twin":
            ref = gathered.at[core, chip_of(item)]
            pltpu.make_async_remote_copy(
                src_ref=ref,
                dst_ref=ref,
                send_sem=twin_send,
                recv_sem=twin_recv.at[order[item]],
                device_id=(y, x, twin, z),
                device_id_type=MESH,
            ).start()
        elif kind == "send":
            node, cut = item
            ref = piece_ref(node, cut)
            step = [0, 0, 0]
            step[way[0]] = way[1] % dims[way[0]]
            ty, tx, tz = shifted(*step)
            pltpu.make_async_remote_copy(
                src_ref=ref,
                dst_ref=ref,
                send_sem=block_send,
                recv_sem=block_recv.at[order[child[0]] * CUTS + cut],
                device_id=(ty, tx, core, tz),
                device_id_type=MESH,
            ).start()
        elif kind == "multiply":
            if first_product:
                load_weight.wait()
                first_product = False
            for node in item:
                drain(gathered.at[twin, chip_of(node)], twin_recv.at[order[node]])
            multiply([chip_of(node) for node in item])
        elif kind == "stats":
            summarize((z + nz - item) % nz)
        else:
            if pieces is None:
                drain(labels_all.at[pl.ds(0, 2 * plane - 1)], label_sem.at[1])
                pieces = label_table()
            place_labels(pieces, (z + nz - item) % nz)

    def merge(ref, slot):
        several = ref[:, slot, :]
        top = jnp.max(several, axis=0, keepdims=True)
        return top + jnp.log(jnp.sum(jnp.exp(several - top), axis=0, keepdims=True))

    filled = lane < part_rows
    insides = []
    for slot in range(pack):
        part = rank * pack + slot
        row_ids = nz * ((part % parts) * part_rows + lane) + part // parts
        inside = (row_ids >= sub_first) & (row_ids < sub_first + sub_len)
        insides.append(jnp.where(inside, 1.0, 0.0))
    contract = (((1,), (1,)), ((), ()))

    stats_in[rank] = stats[rank]
    other_stats = stats_in.at[pl.ds(0, owners - 1)]
    drain(other_stats, stat_sem.at[1])
    merged[...] = jnp.zeros(merged.shape, jnp.float32)
    for slot in range(pack):
        merged[slot : slot + 1, :] = merge(stats_in, slot)
        merged[pack + slot : pack + slot + 1, :] = jnp.sum(
            stats_in[:, pack + slot, :], axis=0, keepdims=True
        )
    sheet = y * nz + z
    merged_in[sheet] = merged[...]
    sheet_peers = sorted(
        [(dy, dz) for dy in range(ny) for dz in range(nz) if (dy, dz) != (0, 0)],
        key=lambda s: -far(s[0], ny) - far(s[1], nz),
    )
    for dy, dz in sheet_peers:
        ty, _, tz = shifted(dy, 0, dz)
        pltpu.make_async_remote_copy(
            src_ref=merged,
            dst_ref=merged_in.at[sheet],
            send_sem=merged_sem.at[0],
            recv_sem=merged_sem.at[1],
            device_id=(ty, x, core, tz),
            device_id_type=MESH,
        ).start()
    other_merged = merged_in.at[pl.ds(0, ny * nz - 1)]
    drain(other_merged, merged_sem.at[1])

    by_seq = jnp.zeros((1, LANES), jnp.float32)
    squares = jnp.zeros((1, LANES), jnp.float32)
    for slot in range(pack):
        log_norm = merge(merged_in, slot)
        picked = jnp.sum(merged_in[:, pack + slot, :], axis=0, keepdims=True)
        gain = jnp.where(filled, picked - log_norm, 0.0)
        by_seq = by_seq + lax.dot_general(
            jnp.broadcast_to(gain, (8, LANES)),
            insides[slot],
            contract,
            precision=lax.Precision.HIGHEST,
            preferred_element_type=jnp.float32,
        )[0:1, :]
        squares = squares + jnp.where(filled, log_norm * log_norm, 0.0)
    squares = jnp.sum(squares, axis=1, keepdims=True)
    sums[...] = jnp.where(lane == seqs, squares, by_seq)
    sums_in[rank] = sums[...]
    for dx in sorted(range(nx), key=lambda d: -far(d, nx)):
        for dc in (0, 1):
            if (dx, dc) == (0, 0):
                continue
            _, tx, _ = shifted(0, dx, 0)
            pltpu.make_async_remote_copy(
                src_ref=sums,
                dst_ref=sums_in.at[rank],
                send_sem=sums_sem.at[0],
                recv_sem=sums_sem.at[1],
                device_id=(y, tx, twin if dc else core, z),
                device_id_type=MESH,
            ).start()
    pair_ids = iota((LANES, LANES), 0)
    select = jnp.zeros((LANES, LANES), jnp.float32)
    seq_ids = iota((LANES, LANES), 1)
    margins = jnp.zeros((1, LANES), jnp.float32)
    for p in range(pairs):
        hit = jnp.where(seq_ids == pairs_ref[2 * p], 1.0, 0.0)
        hit = hit - jnp.where(seq_ids == pairs_ref[2 * p + 1], 1.0, 0.0)
        select = jnp.where(pair_ids == p, hit, select)
        margins = jnp.where(lane == p, margins_ref[p], margins)
    live = functools.reduce(jnp.add, lens).astype(jnp.float32)

    drain(others, parcel_sem.at[0])
    drain(labels_all.at[pl.ds(0, 2 * plane - 1)], label_sem.at[0])
    drain(gathered.at[0, pl.ds(0, plane * nz - 1)], block_send)
    drain(gathered.at[0], twin_send)
    drain(other_stats, stat_sem.at[0])
    drain(other_merged, merged_sem.at[0])
    other_sums = sums_in.at[pl.ds(0, owners - 1)]
    drain(other_sums, sums_sem.at[1])

    row = functools.reduce(jnp.add, [sums_in[k] for k in range(owners)])
    seq_row = jnp.where(lane < seqs, row, 0.0)
    difference = lax.dot_general(
        jnp.broadcast_to(seq_row, (8, LANES)),
        select,
        contract,
        precision=lax.Precision.HIGHEST,
        preferred_element_type=jnp.float32,
    )[0:1, :]
    score = -pref_beta * (difference - margins)
    pair_row = jnp.maximum(score, 0.0) + log_one_plus(jnp.exp(-jnp.abs(score)))
    z_row = zloss_weight * row / live
    out_ref[0:1, :] = seq_row
    out_ref[1:2, :] = pair_row
    out_ref[2:3, :] = z_row
    out_ref[3:8, :] = jnp.zeros((5, LANES), jnp.float32)
    drain(other_sums, sums_sem.at[0])


def split_results(results_ref, seq_out, pair_out, z_out):
    seqs = seq_out.shape[1]
    seq_out[...] = results_ref[0:1, :seqs]
    pair_out[...] = results_ref[1:2, : pair_out.shape[1]]
    z_out[...] = results_ref[2:3, seqs : seqs + 1]


def per_device(dims, hidden, head_weight, labels, lengths, pair_map, ref_margin):
    ny, nx, nz = dims
    plane = ny * nx
    window, width = hidden.shape
    columns = head_weight.shape[1]
    seqs = lengths.shape[0]
    live = seqs * window // 2
    rows = live // nz
    slots = -(-window // (nz * 16)) * 16
    bf16, f32, i32 = jnp.bfloat16, jnp.float32, jnp.int32
    vmem = pltpu.VMEM
    dma = pltpu.SemaphoreType.DMA
    results = pl.pallas_call(
        functools.partial(kernel, dims),
        out_shape=jax.ShapeDtypeStruct((8, LANES), f32),
        in_specs=[
            pl.BlockSpec(memory_space=pl.ANY),
            pl.BlockSpec(memory_space=pl.ANY),
            pl.BlockSpec(memory_space=vmem),
            pl.BlockSpec(memory_space=pltpu.SMEM),
            pl.BlockSpec(memory_space=pltpu.SMEM),
            pl.BlockSpec(memory_space=pltpu.SMEM),
        ],
        out_specs=pl.BlockSpec(memory_space=vmem),
        scratch_shapes=[
            vmem((window, width), bf16),
            vmem((width, columns), bf16),
            vmem((2 * plane, slots, LANES), bf16),
            vmem((2 * plane, slots, LANES), bf16),
            vmem((1, LANES), i32),
            vmem((2 * plane, 1, LANES), i32),
            vmem((2, plane * nz, rows, LANES), bf16),
            vmem((nz, rows, columns), f32),
            vmem((nz, rows, LANES), f32),
            vmem((rows + LANES // 16, LANES), f32),
            vmem((2 * nx, 4, LANES), f32),
            vmem((2 * nx, 4, LANES), f32),
            vmem((4, LANES), f32),
            vmem((ny * nz, 4, LANES), f32),
            vmem((1, LANES), f32),
            vmem((2 * nx, 1, LANES), f32),
            dma((2,)),
            dma((2,)),
            dma((2,)),
            dma(()),
            dma(()),
            dma((CUTS * plane * nz,)),
            dma((plane * nz,)),
            dma((2,)),
            dma((2,)),
            dma((2,)),
        ],
        compiler_params=pltpu.CompilerParams(collective_id=0, has_side_effects=True),
    )(hidden, head_weight, labels.reshape(1, window), lengths, pair_map, ref_margin)
    seq_logps, pair_loss, z_loss = pl.pallas_call(
        split_results,
        out_shape=[jax.ShapeDtypeStruct((1, n), f32) for n in (seqs, seqs // 2, 1)],
        in_specs=[pl.BlockSpec(memory_space=vmem)],
        out_specs=[pl.BlockSpec(memory_space=vmem)] * 3,
    )(results)
    return seq_logps.reshape(seqs), pair_loss.reshape(seqs // 2), z_loss.reshape(())


def solution(mesh):
    nz = mesh.shape["vocab"]
    ny = nx = {32: 4, 8: 2}[mesh.shape["seq"]]
    torus = Mesh(
        mesh.devices.reshape(ny, nx, 2, nz), ("seq_0", "seq_1", "seq_2", "vocab")
    )
    return jax.shard_map(
        functools.partial(per_device, (ny, nx, nz)),
        mesh=torus,
        in_specs=(P(SEQ, None), P(None, SEQ_VOCAB), P(SEQ), P(), P(), P()),
        out_specs=(P(), P(), P()),
        check_vma=False,
    )
```

```python
import functools
import heapq
import math

import jax
import jax.numpy as jnp
from jax import lax
from jax.experimental import pallas as pl
from jax.experimental.pallas import tpu as pltpu
from jax.sharding import Mesh
from jax.sharding import PartitionSpec as P

SEQ = ("seq_0", "seq_1", "seq_2")
SEQ_VOCAB = ("seq_0", "seq_1", "seq_2", "vocab")
MESH = pl.DeviceIdType.MESH

pref_beta = 0.05
zloss_weight = 0.0001

LANES = 128
CHUNK = 4
CUTS = 2
BACKLOG = 1.8
WIRE = 1.33
HOP = 2.2
TWIN = 1.6
ISSUE = 0.012
PAIR = 0.108
PLACE = 0.35
STATS = 0.35

STEPS = [(0, 1), (0, -1), (1, 1), (1, -1), (2, 1), (2, -1)]
WAYS = [
    4, 4, 4, 5, 5, 5, 5, 2, 2, 4, 4, 4, 2, 2, 2, 3, 4, 2, 3, 5, 2, 3, 5, 3, 4, 3, 3, 3, 5, 3, 3, 0,
    0, 4, 0, 4, 0, 5, 0, 0, 4, 0, 2, 0, 5, 0, 0, 0, 2, 2, 0, 2, 3, 3, 3, 3, 0, 3, 4, 3, 5, 0, 5, 1,
    0, 4, 0, 0, 5, 0, 1, 1, 1, 0, 2, 1, 5, 0, 2, 3, 4, 4, 3, 2, 5, 1, 0, 1, 1, 4, 4, 5, 5, 5, 3, 1,
    1, 4, 1, 5, 1, 1, 5, 2, 4, 1, 1, 2, 2, 1, 2, 2, 1, 2, 2, 2, 1, 5, 1, 1, 1, 3, 4, 4, 3, 5, 3,
]


def broadcast_tree(dims):
    nodes = [
        (a, b, c)
        for a in range(dims[0])
        for b in range(dims[1])
        for c in range(dims[2])
        if (a, b, c) != (0, 0, 0)
    ]
    if len(nodes) == len(WAYS):
        return {node: STEPS[way] for node, way in zip(nodes, WAYS)}
    taken = {}
    for node in nodes:
        axis = next(k for k in range(3) if node[k])
        taken[node] = (axis, 1 if node[axis] <= dims[axis] // 2 else -1)
    return taken


def before(node, way, dims):
    place = list(node)
    place[way[0]] = (place[way[0]] - way[1]) % dims[way[0]]
    return tuple(place)


def gather_plan(dims, cuts):
    taken = broadcast_tree(dims)
    children = {}
    for node, way in taken.items():
        children.setdefault(before(node, way, dims), []).append((node, way))

    @functools.cache
    def height(node):
        return max([1 + height(child) for child, _ in children.get(node, [])], default=0)

    @functools.cache
    def weight(node):
        return 1 + sum(weight(child) for child, _ in children.get(node, []))

    wire = WIRE / cuts
    ways = sorted(set(taken.values()))
    ready = {way: [] for way in ways}
    free = {way: 0.0 for way in ways}
    left = {way: cuts * sum(w == way for w in taken.values()) for way in ways}
    arrivals = [(0.0, cut, ((0, 0, 0), cut)) for cut in range(cuts)]
    count = cuts
    now = 0.0
    plan = []
    arrived = {}
    waiting = {}
    multiplied = 0
    cost = PAIR * CHUNK
    ranks = sorted(range(dims[2]), key=lambda dz: (min(dz, dims[2] - dz), dz))
    places = list(ranks)
    missing = {dz: dims[0] * dims[1] for dz in ranks}
    finished = []

    def multiply(nodes):
        plan.append(("multiply", tuple(nodes), None, None))
        for node in nodes:
            del waiting[node]
            missing[node[2]] -= 1
            if not missing[node[2]]:
                finished.append(node[2])

    def urgency(piece):
        node, cut = piece
        return (-height(node), -weight(node), ranks.index(node[2]), cut, node)

    while arrivals or waiting:
        while arrivals and arrivals[0][0] <= now:
            piece = heapq.heappop(arrivals)[2]
            node, cut = piece
            plan.append(("wait", piece, None, None))
            now += ISSUE
            for child, way in children.get(node, []):
                ready[way].append((child, cut))
            arrived[node] = arrived.get(node, 0) + 1
            if arrived[node] == cuts:
                plan.append(("twin", node, None, None))
                now += ISSUE
                waiting[node] = now + TWIN
        for way in ways:
            while ready[way] and free[way] - now < BACKLOG - 0.5 * wire:
                ready[way].sort(key=urgency)
                piece = ready[way].pop(0)
                free[way] = max(now, free[way]) + wire
                left[way] -= 1
                plan.append(("send", (before(piece[0], way, dims), piece[1]), piece, way))
                now += ISSUE
                heapq.heappush(arrivals, (free[way] + HOP, count, piece))
                count += 1
        if arrivals and arrivals[0][0] <= now:
            continue
        coming = arrivals[0][0] if arrivals else math.inf
        queued = min([free[way] - now for way in ways if left[way]], default=math.inf)
        there = [node for node, when in waiting.items() if when <= now]
        there.sort(key=lambda node: ranks.index(node[2]))
        if finished and finished[0] not in places:
            if queued >= STATS or coming >= now + STATS:
                plan.append(("stats", finished.pop(0), None, None))
                now += STATS
                continue
        if len(there) >= CHUNK and (queued >= cost or coming >= now + cost or len(waiting) > 32):
            multiply(there[:CHUNK])
            multiplied += CHUNK
            now += cost
            continue
        if places and multiplied >= 2 * CHUNK:
            if queued >= PLACE or coming >= now + PLACE:
                plan.append(("place", places.pop(0), None, None))
                now += PLACE
                continue
        later = [coming]
        later += [free[way] - BACKLOG + 0.5 * wire for way in ways if ready[way]]
        if len(waiting) >= CHUNK:
            later.append(max(sorted(waiting.values())[CHUNK - 1], now + 0.05))
        if min(later) == math.inf:
            multiply(list(waiting)[:CHUNK])
            now += cost
            continue
        now = max(now + 1e-6, min(later))
    for dz in places:
        plan.append(("place", dz, None, None))
    for dz in finished:
        plan.append(("stats", dz, None, None))
    return plan


def log_one_plus(u):
    w = u / (2.0 + u)
    square = w * w
    total = jnp.full_like(w, 1.0 / 17.0)
    for odd in (15, 13, 11, 9, 7, 5, 3, 1):
        total = total * square + 1.0 / odd
    return 2.0 * w * total


def iota(shape, dim):
    return lax.broadcasted_iota(jnp.int32, shape, dim)


def scatter_scalars(ids, values):
    out = jnp.zeros(ids.shape, jnp.int32)
    for k, value in enumerate(values):
        out = jnp.where(ids == k, value, out)
    return out


def sums_before(ids, values):
    out = jnp.zeros(ids.shape, jnp.int32)
    for k, value in enumerate(values):
        out = out + jnp.where(ids > k, value, 0)
    return out


def kernel(
    dims,
    hidden_hbm,
    weight_hbm,
    labels_hbm,
    lengths_hbm,
    pairs_hbm,
    margins_hbm,
    out_ref,
    labels_ref,
    lengths_ref,
    pairs_ref,
    margins_ref,
    hidden,
    weight,
    parcels,
    received,
    label_row,
    labels_all,
    gathered,
    scores,
    label_place,
    packed,
    stats,
    stats_in,
    merged,
    merged_in,
    sums,
    sums_in,
    load_sem,
    parcel_sem,
    label_sem,
    block_send,
    twin_send,
    block_recv,
    twin_recv,
    stat_sem,
    merged_sem,
    sums_sem,
):
    ny, nx, nz = dims
    plane = ny * nx
    seqs = lengths_ref.shape[0]
    pairs = margins_ref.shape[0]
    window = hidden.shape[0]
    slots = parcels.shape[1]
    rows = gathered.shape[2]
    columns = weight.shape[1]
    part_rows = 15 * LANES // 16
    parts = rows // part_rows
    pack = nz // nx
    owners = 2 * nx
    y, x = lax.axis_index("seq_0"), lax.axis_index("seq_1")
    core, z = lax.axis_index("seq_2"), lax.axis_index("vocab")
    here = y * nx + x
    mine = here * 2 + core
    twin = 1 - core
    rank = x * 2 + core

    def shifted(dy, dx, dz):
        return ((y + dy) % ny, (x + dx) % nx, (z + dz) % nz)

    def chip_of(node):
        cy, cx, cz = shifted(-node[0] + ny, -node[1] + nx, -node[2] + nz)
        return (cy * nx + cx) * nz + cz

    load_hidden = pltpu.make_async_copy(hidden_hbm, hidden, load_sem.at[0])
    load_weight = pltpu.make_async_copy(weight_hbm, weight, load_sem.at[1])
    load_hidden.start()
    small = [(lengths_hbm, lengths_ref), (labels_hbm, labels_ref)]
    small += [(pairs_hbm, pairs_ref), (margins_hbm, margins_ref)]
    load_small = [
        pltpu.make_async_copy(source, target, load_sem.at[2 + k])
        for k, (source, target) in enumerate(small)
    ]
    for copy in load_small:
        copy.start()

    far = lambda n, size: min(n, size - n)
    plane_steps = sorted(
        [(a, b) for a in range(ny) for b in range(nx)],
        key=lambda s: -(far(s[0], ny) + far(s[1], nx)),
    )
    plane_peers = [(a, b, c) for a, b in plane_steps for c in (0, 1) if (a, b, c) != (0, 0, 0)]

    def peer_of(step):
        py, px, _ = shifted(step[0], step[1], 0)
        pc = twin if step[2] else core
        return py, px, pc

    barrier = pltpu.get_barrier_semaphore()
    for step in plane_peers:
        py, px, pc = peer_of(step)
        pl.semaphore_signal(barrier, inc=1, device_id=(py, px, pc, z), device_id_type=MESH)
    z_steps = sorted({1 % nz, nz - 1} - {0})
    for dz in z_steps:
        pl.semaphore_signal(
            barrier, inc=1, device_id=(y, x, core, (z + dz) % nz), device_id_type=MESH
        )

    for copy in load_small:
        copy.wait()
    lens = [lengths_ref[s] for s in range(seqs)]
    own_first = jnp.int32(0)
    for s in range(seqs - 1):
        own_first = own_first + jnp.where(mine > s, lens[s], 0)
    own_place = nz * iota((slots, window), 0) + ((z - own_first) & (nz - 1))
    choose = jnp.where(own_place == iota((slots, window), 1), 1.0, 0.0).astype(jnp.bfloat16)

    label_row[...] = jnp.zeros(label_row.shape, jnp.int32)
    label_row[0:1, 0:window] = labels_ref[...]
    labels_all[mine] = label_row[...]
    load_hidden.wait()
    load_weight.start()
    chosen = jnp.dot(choose, hidden[...], preferred_element_type=jnp.float32)
    chosen = chosen.astype(jnp.bfloat16)
    for j in range(2 * plane):
        parcels[j] = chosen[:, j * LANES : (j + 1) * LANES]
    received[mine] = parcels[mine]

    pl.semaphore_wait(barrier, len(plane_peers) + len(z_steps))

    for step in plane_peers:
        py, px, pc = peer_of(step)
        pltpu.make_async_remote_copy(
            src_ref=parcels.at[(py * nx + px) * 2 + pc],
            dst_ref=received.at[mine],
            send_sem=parcel_sem.at[0],
            recv_sem=parcel_sem.at[1],
            device_id=(py, px, pc, z),
            device_id_type=MESH,
        ).start()
    for step in plane_peers:
        py, px, pc = peer_of(step)
        pltpu.make_async_remote_copy(
            src_ref=label_row,
            dst_ref=labels_all.at[mine],
            send_sem=label_sem.at[0],
            recv_sem=label_sem.at[1],
            device_id=(py, px, pc, z),
            device_id_type=MESH,
        ).start()
    slot_ids = iota((1, seqs * slots), 1)
    slot_seq = slot_ids // slots
    first = sums_before(slot_seq, lens)
    place = nz * (slot_ids % slots) + ((z - first) & (nz - 1))
    row_of_slot = jnp.where(
        place < scatter_scalars(slot_seq, lens), (first + place - z) // nz, -1
    )
    scores[...] = jnp.zeros(scores.shape, jnp.float32)
    compact = jnp.where(iota((rows, seqs * slots), 0) == row_of_slot, 1.0, 0.0)
    compact = compact.astype(jnp.bfloat16)
    others = received.at[pl.ds(0, 2 * plane - 1)]
    pltpu.make_async_copy(others, others, parcel_sem.at[1]).wait()
    block = jnp.dot(
        compact,
        received[...].reshape(seqs * slots, LANES),
        preferred_element_type=jnp.float32,
    )
    own_chip = here * nz + z
    gathered[core, own_chip] = block.astype(jnp.bfloat16)

    lane = iota((1, LANES), 1)
    lane_first = sums_before(lane, lens)
    lane_len = scatter_scalars(lane, lens)
    sub = iota((LANES, LANES), 0)
    sub_first = sums_before(sub, lens)
    sub_len = scatter_scalars(sub, lens)

    def label_table():
        row_ids = iota((LANES, LANES), 0)
        table = jnp.zeros((LANES, LANES), jnp.int32)
        for s in range(seqs):
            table = jnp.where(row_ids == s, labels_all[s], table)
        col_first = (mine * nz + z) * columns
        local = table - col_first
        code = jnp.where((local >= 0) & (local < columns), local + 1, 0)
        pieces = [code // 16, code % 16, sub_first // 16, sub_first % 16]
        return [piece.astype(jnp.float32).astype(jnp.bfloat16) for piece in pieces]

    def place_labels(pieces, zz):
        ids = nz * iota((rows, LANES), 0) + zz
        member = (ids >= lane_first) & (ids < lane_first + lane_len)
        member = jnp.where(member, 1.0, 0.0).astype(jnp.bfloat16)
        high, low, first_high, first_low = [
            jnp.dot(member, piece, preferred_element_type=jnp.float32) for piece in pieces
        ]
        position = ids.astype(jnp.float32) - (16.0 * first_high + first_low)
        at = position == iota((rows, LANES), 1).astype(jnp.float32)
        code = jnp.sum(jnp.where(at, 16.0 * high + low, 0.0), axis=1, keepdims=True)
        label_place[zz] = jnp.broadcast_to(code - 1.0, (rows, LANES))

    def multiply(chips):
        products = []
        for chip in chips:
            depth = pl.multiple_of((chip // nz) * (2 * LANES), 2 * LANES)
            pair = jnp.concatenate([gathered[0, chip], gathered[1, chip]], axis=1)
            product = jnp.dot(
                pair, weight[pl.ds(depth, 2 * LANES), :], preferred_element_type=jnp.float32
            )
            products.append((chip % nz, product))
        for zz, product in products:
            scores[zz] = scores[zz] + product

    spot = iota((rows, LANES), 1)

    def summarize(zz):
        tiles = [scores[zz, :, k : k + LANES] for k in range(0, columns, LANES)]
        top = jnp.max(functools.reduce(jnp.maximum, tiles), axis=1, keepdims=True)
        total = functools.reduce(jnp.add, [jnp.exp(tile - top) for tile in tiles])
        total = jnp.sum(total, axis=1, keepdims=True)
        code = label_place[zz]
        picked = functools.reduce(
            jnp.add,
            [
                jnp.where(code - float(k * LANES) == spot.astype(jnp.float32), tile, 0.0)
                for k, tile in enumerate(tiles)
            ],
        )
        picked = jnp.sum(picked, axis=1, keepdims=True)
        packed[0:rows, :] = jnp.where(spot == 0, top + jnp.log(total), picked)
        for part in range(parts):
            flat = packed[part * part_rows : part * part_rows + LANES, :].T
            slot = part % pack
            owner = zz * (parts // pack) + part // pack
            stats[owner, slot : slot + 1, :] = flat[0:1, :]
            stats[owner, pack + slot : pack + slot + 1, :] = flat[1:2, :]
            if slot == pack - 1:

                @pl.when(owner != rank)
                def _():
                    pltpu.make_async_remote_copy(
                        src_ref=stats.at[owner],
                        dst_ref=stats_in.at[rank],
                        send_sem=stat_sem.at[0],
                        recv_sem=stat_sem.at[1],
                        device_id=(y, owner // 2, owner % 2, z),
                        device_id_type=MESH,
                    ).start()

    packed[rows:, :] = jnp.zeros((LANES - part_rows, LANES), jnp.float32)
    edges = [0, LANES, rows] if CUTS == 2 else [0, rows]
    plan = gather_plan(dims, CUTS)
    order = {}
    for kind, item, _, _ in plan:
        if kind == "twin":
            order[item] = len(order)

    def piece_ref(node, cut):
        return gathered.at[core, chip_of(node), pl.ds(edges[cut], edges[cut + 1] - edges[cut])]

    def drain(ref, sem):
        pltpu.make_async_copy(ref, ref, sem).wait()

    pieces = None
    first_product = True
    for kind, item, child, way in plan:
        if kind == "wait":
            node, cut = item
            if node != (0, 0, 0):
                drain(piece_ref(node, cut), block_recv.at[order[node] * CUTS + cut])
        elif kind == "twin":
            ref = gathered.at[core, chip_of(item)]
            pltpu.make_async_remote_copy(
                src_ref=ref,
                dst_ref=ref,
                send_sem=twin_send,
                recv_sem=twin_recv.at[order[item]],
                device_id=(y, x, twin, z),
                device_id_type=MESH,
            ).start()
        elif kind == "send":
            node, cut = item
            ref = piece_ref(node, cut)
            step = [0, 0, 0]
            step[way[0]] = way[1] % dims[way[0]]
            ty, tx, tz = shifted(*step)
            pltpu.make_async_remote_copy(
                src_ref=ref,
                dst_ref=ref,
                send_sem=block_send,
                recv_sem=block_recv.at[order[child[0]] * CUTS + cut],
                device_id=(ty, tx, core, tz),
                device_id_type=MESH,
            ).start()
        elif kind == "multiply":
            if first_product:
                load_weight.wait()
                first_product = False
            for node in item:
                drain(gathered.at[twin, chip_of(node)], twin_recv.at[order[node]])
            multiply([chip_of(node) for node in item])
        elif kind == "stats":
            summarize((z + nz - item) % nz)
        else:
            if pieces is None:
                drain(labels_all.at[pl.ds(0, 2 * plane - 1)], label_sem.at[1])
                pieces = label_table()
            place_labels(pieces, (z + nz - item) % nz)

    def merge(ref, slot):
        several = ref[:, slot, :]
        top = jnp.max(several, axis=0, keepdims=True)
        return top + jnp.log(jnp.sum(jnp.exp(several - top), axis=0, keepdims=True))

    pair_ids = iota((LANES, LANES), 0)
    select = jnp.zeros((LANES, LANES), jnp.float32)
    seq_ids = iota((LANES, LANES), 1)
    margins = jnp.zeros((1, LANES), jnp.float32)
    for p in range(pairs):
        hit = jnp.where(seq_ids == pairs_ref[2 * p], 1.0, 0.0)
        hit = hit - jnp.where(seq_ids == pairs_ref[2 * p + 1], 1.0, 0.0)
        select = jnp.where(pair_ids == p, hit, select)
        margins = jnp.where(lane == p, margins_ref[p], margins)
    filled = lane < part_rows
    insides = []
    for slot in range(pack):
        part = rank * pack + slot
        row_ids = nz * ((part % parts) * part_rows + lane) + part // parts
        inside = (row_ids >= sub_first) & (row_ids < sub_first + sub_len)
        inside = jnp.where(inside, 1.0, 0.0)
        by_pair = jnp.dot(select, inside, preferred_element_type=jnp.float32)
        insides.append(jnp.concatenate([inside, by_pair], axis=0))
    contract = (((1,), (1,)), ((), ()))

    stats_in[rank] = stats[rank]
    other_stats = stats_in.at[pl.ds(0, owners - 1)]
    drain(other_stats, stat_sem.at[1])
    merged[...] = jnp.zeros(merged.shape, jnp.float32)
    for slot in range(pack):
        merged[slot : slot + 1, :] = merge(stats_in, slot)
        merged[pack + slot : pack + slot + 1, :] = jnp.sum(
            stats_in[:, pack + slot, :], axis=0, keepdims=True
        )
    sheet = y * nz + z
    merged_in[sheet] = merged[...]
    sheet_peers = sorted(
        [(dy, dz) for dy in range(ny) for dz in range(nz) if (dy, dz) != (0, 0)],
        key=lambda s: -far(s[0], ny) - far(s[1], nz),
    )
    for dy, dz in sheet_peers:
        ty, _, tz = shifted(dy, 0, dz)
        pltpu.make_async_remote_copy(
            src_ref=merged,
            dst_ref=merged_in.at[sheet],
            send_sem=merged_sem.at[0],
            recv_sem=merged_sem.at[1],
            device_id=(ty, x, core, tz),
            device_id_type=MESH,
        ).start()
    other_merged = merged_in.at[pl.ds(0, ny * nz - 1)]
    drain(other_merged, merged_sem.at[1])

    totals = jnp.zeros((1, 2 * LANES), jnp.float32)
    squares = jnp.zeros((1, LANES), jnp.float32)
    for slot in range(pack):
        log_norm = merge(merged_in, slot)
        picked = jnp.sum(merged_in[:, pack + slot, :], axis=0, keepdims=True)
        gain = jnp.where(filled, picked - log_norm, 0.0)
        totals = totals + lax.dot_general(
            jnp.broadcast_to(gain, (8, LANES)),
            insides[slot],
            contract,
            precision=lax.Precision.HIGHEST,
            preferred_element_type=jnp.float32,
        )[0:1, :]
        squares = squares + jnp.where(filled, log_norm * log_norm, 0.0)
    squares = jnp.sum(squares, axis=1, keepdims=True)
    sums[0:1, :] = jnp.where(lane == seqs, squares, totals[:, :LANES])
    sums[1:2, :] = totals[:, LANES:]
    sums_in[rank] = sums[...]
    for dx in sorted(range(nx), key=lambda d: -far(d, nx)):
        for dc in (0, 1):
            if (dx, dc) == (0, 0):
                continue
            _, tx, _ = shifted(0, dx, 0)
            pltpu.make_async_remote_copy(
                src_ref=sums,
                dst_ref=sums_in.at[rank],
                send_sem=sums_sem.at[0],
                recv_sem=sums_sem.at[1],
                device_id=(y, tx, twin if dc else core, z),
                device_id_type=MESH,
            ).start()
    live = functools.reduce(jnp.add, lens).astype(jnp.float32)

    drain(others, parcel_sem.at[0])
    drain(labels_all.at[pl.ds(0, 2 * plane - 1)], label_sem.at[0])
    drain(gathered.at[0, pl.ds(0, plane * nz - 1)], block_send)
    drain(gathered.at[0], twin_send)
    drain(other_stats, stat_sem.at[0])
    drain(other_merged, merged_sem.at[0])
    other_sums = sums_in.at[pl.ds(0, owners - 1)]
    drain(other_sums, sums_sem.at[1])

    table = functools.reduce(jnp.add, [sums_in[k] for k in range(owners)])
    row, difference = table[0:1, :], table[1:2, :]
    score = -pref_beta * (difference - margins)
    pair_row = jnp.maximum(score, 0.0) + log_one_plus(jnp.exp(-jnp.abs(score)))
    z_row = zloss_weight * row / live
    out_ref[0:1, :] = row
    out_ref[1:2, :] = pair_row
    out_ref[2:3, :] = z_row
    out_ref[3:8, :] = jnp.zeros((5, LANES), jnp.float32)
    drain(other_sums, sums_sem.at[0])


def split_results(results_ref, seq_out, pair_out, z_out):
    seqs = seq_out.shape[1]
    seq_out[...] = results_ref[0:1, :seqs]
    pair_out[...] = results_ref[1:2, : pair_out.shape[1]]
    z_out[...] = results_ref[2:3, seqs : seqs + 1]


def per_device(dims, hidden, head_weight, labels, lengths, pair_map, ref_margin):
    ny, nx, nz = dims
    plane = ny * nx
    window, width = hidden.shape
    columns = head_weight.shape[1]
    seqs = lengths.shape[0]
    live = seqs * window // 2
    rows = live // nz
    slots = -(-window // (nz * 16)) * 16
    bf16, f32, i32 = jnp.bfloat16, jnp.float32, jnp.int32
    vmem = pltpu.VMEM
    dma = pltpu.SemaphoreType.DMA
    results = pl.pallas_call(
        functools.partial(kernel, dims),
        out_shape=jax.ShapeDtypeStruct((8, LANES), f32),
        in_specs=[
            pl.BlockSpec(memory_space=pl.ANY),
        ]
        * 6,
        out_specs=pl.BlockSpec(memory_space=vmem),
        scratch_shapes=[
            vmem((1, window), i32),
            pltpu.SMEM((seqs,), i32),
            pltpu.SMEM((seqs,), i32),
            pltpu.SMEM((seqs // 2,), f32),
            vmem((window, width), bf16),
            vmem((width, columns), bf16),
            vmem((2 * plane, slots, LANES), bf16),
            vmem((2 * plane, slots, LANES), bf16),
            vmem((1, LANES), i32),
            vmem((2 * plane, 1, LANES), i32),
            vmem((2, plane * nz, rows, LANES), bf16),
            vmem((nz, rows, columns), f32),
            vmem((nz, rows, LANES), f32),
            vmem((rows + LANES // 16, LANES), f32),
            vmem((2 * nx, 4, LANES), f32),
            vmem((2 * nx, 4, LANES), f32),
            vmem((4, LANES), f32),
            vmem((ny * nz, 4, LANES), f32),
            vmem((2, LANES), f32),
            vmem((2 * nx, 2, LANES), f32),
            dma((6,)),
            dma((2,)),
            dma((2,)),
            dma(()),
            dma(()),
            dma((CUTS * plane * nz,)),
            dma((plane * nz,)),
            dma((2,)),
            dma((2,)),
            dma((2,)),
        ],
        compiler_params=pltpu.CompilerParams(collective_id=0, has_side_effects=True),
    )(hidden, head_weight, labels.reshape(1, window), lengths, pair_map, ref_margin)
    seq_logps, pair_loss, z_loss = pl.pallas_call(
        split_results,
        out_shape=[jax.ShapeDtypeStruct((1, n), f32) for n in (seqs, seqs // 2, 1)],
        in_specs=[pl.BlockSpec(memory_space=vmem)],
        out_specs=[pl.BlockSpec(memory_space=vmem)] * 3,
    )(results)
    return seq_logps.reshape(seqs), pair_loss.reshape(seqs // 2), z_loss.reshape(())


def solution(mesh):
    nz = mesh.shape["vocab"]
    ny = nx = {32: 4, 8: 2}[mesh.shape["seq"]]
    torus = Mesh(
        mesh.devices.reshape(ny, nx, 2, nz), ("seq_0", "seq_1", "seq_2", "vocab")
    )
    return jax.shard_map(
        functools.partial(per_device, (ny, nx, nz)),
        mesh=torus,
        in_specs=(P(SEQ, None), P(None, SEQ_VOCAB), P(SEQ), P(), P(), P()),
        out_specs=(P(), P(), P()),
        check_vma=False,
    )
```

```python
import functools
import heapq
import math

import jax
import jax.numpy as jnp
from jax import lax
from jax.experimental import pallas as pl
from jax.experimental.pallas import tpu as pltpu
from jax.sharding import Mesh
from jax.sharding import PartitionSpec as P

SEQ = ("seq_0", "seq_1", "seq_2")
SEQ_VOCAB = ("seq_0", "seq_1", "seq_2", "vocab")
MESH = pl.DeviceIdType.MESH

pref_beta = 0.05
zloss_weight = 0.0001

LANES = 128
CHUNK = 4
CUTS = 2
BACKLOG = 1.8
WIRE = 1.33
HOP = 2.2
TWIN = 1.6
ISSUE = 0.012
PAIR = 0.108
PLACE = 0.35
STATS = 0.35

STEPS = [(0, 1), (0, -1), (1, 1), (1, -1), (2, 1), (2, -1)]
WAYS = [
    4, 4, 4, 5, 5, 5, 5, 2, 2, 4, 4, 4, 2, 2, 2, 3, 4, 2, 3, 5, 2, 3, 5, 3, 4, 3, 3, 3, 5, 3, 3, 0,
    0, 4, 0, 4, 0, 5, 0, 0, 4, 0, 2, 0, 5, 0, 0, 0, 2, 2, 0, 2, 3, 3, 3, 3, 0, 3, 4, 3, 5, 0, 5, 1,
    0, 4, 0, 0, 5, 0, 1, 1, 1, 0, 2, 1, 5, 0, 2, 3, 4, 4, 3, 2, 5, 1, 0, 1, 1, 4, 4, 5, 5, 5, 3, 1,
    1, 4, 1, 5, 1, 1, 5, 2, 4, 1, 1, 2, 2, 1, 2, 2, 1, 2, 2, 2, 1, 5, 1, 1, 1, 3, 4, 4, 3, 5, 3,
]


def broadcast_tree(dims):
    nodes = [
        (a, b, c)
        for a in range(dims[0])
        for b in range(dims[1])
        for c in range(dims[2])
        if (a, b, c) != (0, 0, 0)
    ]
    if len(nodes) == len(WAYS):
        return {node: STEPS[way] for node, way in zip(nodes, WAYS)}
    taken = {}
    for node in nodes:
        axis = next(k for k in range(3) if node[k])
        taken[node] = (axis, 1 if node[axis] <= dims[axis] // 2 else -1)
    return taken


def before(node, way, dims):
    place = list(node)
    place[way[0]] = (place[way[0]] - way[1]) % dims[way[0]]
    return tuple(place)


def gather_plan(dims, cuts):
    taken = broadcast_tree(dims)
    children = {}
    for node, way in taken.items():
        children.setdefault(before(node, way, dims), []).append((node, way))

    @functools.cache
    def height(node):
        return max([1 + height(child) for child, _ in children.get(node, [])], default=0)

    @functools.cache
    def weight(node):
        return 1 + sum(weight(child) for child, _ in children.get(node, []))

    wire = WIRE / cuts
    ways = sorted(set(taken.values()))
    ready = {way: [] for way in ways}
    free = {way: 0.0 for way in ways}
    left = {way: cuts * sum(w == way for w in taken.values()) for way in ways}
    arrivals = [(0.0, cut, ((0, 0, 0), cut)) for cut in range(cuts)]
    count = cuts
    now = 0.0
    plan = []
    arrived = {}
    waiting = {}
    multiplied = 0
    cost = PAIR * CHUNK
    ranks = sorted(range(dims[2]), key=lambda dz: (min(dz, dims[2] - dz), dz))
    places = list(ranks)
    missing = {dz: dims[0] * dims[1] for dz in ranks}
    finished = []

    def multiply(nodes):
        plan.append(("multiply", tuple(nodes), None, None))
        for node in nodes:
            del waiting[node]
            missing[node[2]] -= 1
            if not missing[node[2]]:
                finished.append(node[2])

    def urgency(piece):
        node, cut = piece
        return (-height(node), -weight(node), ranks.index(node[2]), cut, node)

    while arrivals or waiting:
        while arrivals and arrivals[0][0] <= now:
            piece = heapq.heappop(arrivals)[2]
            node, cut = piece
            plan.append(("wait", piece, None, None))
            now += ISSUE
            for child, way in children.get(node, []):
                ready[way].append((child, cut))
            arrived[node] = arrived.get(node, 0) + 1
            if arrived[node] == cuts:
                plan.append(("twin", node, None, None))
                now += ISSUE
                waiting[node] = now + TWIN
        for way in ways:
            while ready[way] and free[way] - now < BACKLOG - 0.5 * wire:
                ready[way].sort(key=urgency)
                piece = ready[way].pop(0)
                free[way] = max(now, free[way]) + wire
                left[way] -= 1
                plan.append(("send", (before(piece[0], way, dims), piece[1]), piece, way))
                now += ISSUE
                heapq.heappush(arrivals, (free[way] + HOP, count, piece))
                count += 1
        if arrivals and arrivals[0][0] <= now:
            continue
        coming = arrivals[0][0] if arrivals else math.inf
        queued = min([free[way] - now for way in ways if left[way]], default=math.inf)
        there = [node for node, when in waiting.items() if when <= now]
        there.sort(key=lambda node: ranks.index(node[2]))
        if finished and finished[0] not in places:
            if queued >= STATS or coming >= now + STATS:
                plan.append(("stats", finished.pop(0), None, None))
                now += STATS
                continue
        if len(there) >= CHUNK and (queued >= cost or coming >= now + cost or len(waiting) > 32):
            multiply(there[:CHUNK])
            multiplied += CHUNK
            now += cost
            continue
        if places and multiplied >= 2 * CHUNK:
            if queued >= PLACE or coming >= now + PLACE:
                plan.append(("place", places.pop(0), None, None))
                now += PLACE
                continue
        later = [coming]
        later += [free[way] - BACKLOG + 0.5 * wire for way in ways if ready[way]]
        if len(waiting) >= CHUNK:
            later.append(max(sorted(waiting.values())[CHUNK - 1], now + 0.05))
        if min(later) == math.inf:
            multiply(list(waiting)[:CHUNK])
            now += cost
            continue
        now = max(now + 1e-6, min(later))
    for dz in places:
        plan.append(("place", dz, None, None))
    for dz in finished:
        plan.append(("stats", dz, None, None))
    return plan


def log_one_plus(u):
    w = u / (2.0 + u)
    square = w * w
    total = jnp.full_like(w, 1.0 / 17.0)
    for odd in (15, 13, 11, 9, 7, 5, 3, 1):
        total = total * square + 1.0 / odd
    return 2.0 * w * total


def iota(shape, dim):
    return lax.broadcasted_iota(jnp.int32, shape, dim)


def scatter_scalars(ids, values):
    out = jnp.zeros(ids.shape, jnp.int32)
    for k, value in enumerate(values):
        out = jnp.where(ids == k, value, out)
    return out


def sums_before(ids, values):
    out = jnp.zeros(ids.shape, jnp.int32)
    for k, value in enumerate(values):
        out = out + jnp.where(ids > k, value, 0)
    return out


def kernel(
    dims,
    hidden_hbm,
    weight_hbm,
    labels_hbm,
    lengths_hbm,
    pairs_hbm,
    margins_hbm,
    out_ref,
    labels_ref,
    lengths_ref,
    pairs_ref,
    margins_ref,
    hidden,
    weight,
    parcels,
    received,
    label_row,
    labels_all,
    gathered,
    scores,
    label_place,
    packed,
    stats,
    stats_in,
    merged,
    merged_in,
    sums,
    sums_in,
    load_sem,
    parcel_sem,
    label_sem,
    block_send,
    twin_send,
    block_recv,
    twin_recv,
    stat_sem,
    merged_sem,
    sums_sem,
):
    ny, nx, nz = dims
    plane = ny * nx
    seqs = lengths_ref.shape[0]
    pairs = margins_ref.shape[0]
    window = hidden.shape[0]
    slots = parcels.shape[1]
    rows = gathered.shape[2]
    columns = weight.shape[1]
    part_rows = 15 * LANES // 16
    parts = rows // part_rows
    pack = nz // nx
    owners = 2 * nx
    y, x = lax.axis_index("seq_0"), lax.axis_index("seq_1")
    core, z = lax.axis_index("seq_2"), lax.axis_index("vocab")
    here = y * nx + x
    mine = here * 2 + core
    twin = 1 - core
    rank = x * 2 + core

    def shifted(dy, dx, dz):
        return ((y + dy) % ny, (x + dx) % nx, (z + dz) % nz)

    def chip_of(node):
        cy, cx, cz = shifted(-node[0] + ny, -node[1] + nx, -node[2] + nz)
        return (cy * nx + cx) * nz + cz

    far = lambda n, size: min(n, size - n)
    plane_steps = sorted(
        [(a, b) for a in range(ny) for b in range(nx)],
        key=lambda s: -(far(s[0], ny) + far(s[1], nx)),
    )
    plane_peers = [(a, b, c) for a, b in plane_steps for c in (0, 1) if (a, b, c) != (0, 0, 0)]

    def peer_of(step):
        py, px, _ = shifted(step[0], step[1], 0)
        pc = twin if step[2] else core
        return py, px, pc

    barrier = pltpu.get_barrier_semaphore()
    for step in plane_peers:
        py, px, pc = peer_of(step)
        pl.semaphore_signal(barrier, inc=1, device_id=(py, px, pc, z), device_id_type=MESH)
    z_steps = sorted({1 % nz, nz - 1} - {0})
    for dz in z_steps:
        pl.semaphore_signal(
            barrier, inc=1, device_id=(y, x, core, (z + dz) % nz), device_id_type=MESH
        )

    load_hidden = pltpu.make_async_copy(hidden_hbm, hidden, load_sem.at[0])
    load_weight = pltpu.make_async_copy(weight_hbm, weight, load_sem.at[1])
    load_hidden.start()
    small = [(lengths_hbm, lengths_ref), (labels_hbm, labels_ref)]
    small += [(pairs_hbm, pairs_ref), (margins_hbm, margins_ref)]
    load_small = [
        pltpu.make_async_copy(source, target, load_sem.at[2 + k])
        for k, (source, target) in enumerate(small)
    ]
    for copy in load_small:
        copy.start()

    for copy in load_small:
        copy.wait()
    lens = [lengths_ref[s] for s in range(seqs)]
    own_first = jnp.int32(0)
    for s in range(seqs - 1):
        own_first = own_first + jnp.where(mine > s, lens[s], 0)
    own_place = nz * iota((slots, window), 0) + ((z - own_first) & (nz - 1))
    choose = jnp.where(own_place == iota((slots, window), 1), 1.0, 0.0).astype(jnp.bfloat16)

    label_row[...] = jnp.zeros(label_row.shape, jnp.int32)
    label_row[0:1, 0:window] = labels_ref[...]
    labels_all[mine] = label_row[...]
    load_hidden.wait()
    load_weight.start()
    chosen = jnp.dot(choose, hidden[...], preferred_element_type=jnp.float32)
    chosen = chosen.astype(jnp.bfloat16)
    for j in range(2 * plane):
        parcels[j] = chosen[:, j * LANES : (j + 1) * LANES]
    received[mine] = parcels[mine]

    pl.semaphore_wait(barrier, len(plane_peers) + len(z_steps))

    for step in plane_peers:
        py, px, pc = peer_of(step)
        pltpu.make_async_remote_copy(
            src_ref=parcels.at[(py * nx + px) * 2 + pc],
            dst_ref=received.at[mine],
            send_sem=parcel_sem.at[0],
            recv_sem=parcel_sem.at[1],
            device_id=(py, px, pc, z),
            device_id_type=MESH,
        ).start()
    for step in plane_peers:
        py, px, pc = peer_of(step)
        pltpu.make_async_remote_copy(
            src_ref=label_row,
            dst_ref=labels_all.at[mine],
            send_sem=label_sem.at[0],
            recv_sem=label_sem.at[1],
            device_id=(py, px, pc, z),
            device_id_type=MESH,
        ).start()
    slot_ids = iota((1, seqs * slots), 1)
    slot_seq = slot_ids // slots
    first = sums_before(slot_seq, lens)
    place = nz * (slot_ids % slots) + ((z - first) & (nz - 1))
    row_of_slot = jnp.where(
        place < scatter_scalars(slot_seq, lens), (first + place - z) // nz, -1
    )
    scores[...] = jnp.zeros(scores.shape, jnp.float32)
    compact = jnp.where(iota((rows, seqs * slots), 0) == row_of_slot, 1.0, 0.0)
    compact = compact.astype(jnp.bfloat16)
    others = received.at[pl.ds(0, 2 * plane - 1)]
    pltpu.make_async_copy(others, others, parcel_sem.at[1]).wait()
    block = jnp.dot(
        compact,
        received[...].reshape(seqs * slots, LANES),
        preferred_element_type=jnp.float32,
    )
    own_chip = here * nz + z
    gathered[core, own_chip] = block.astype(jnp.bfloat16)

    lane = iota((1, LANES), 1)
    lane_first = sums_before(lane, lens)
    lane_len = scatter_scalars(lane, lens)
    sub = iota((LANES, LANES), 0)
    sub_first = sums_before(sub, lens)
    sub_len = scatter_scalars(sub, lens)

    def label_table():
        row_ids = iota((LANES, LANES), 0)
        table = jnp.zeros((LANES, LANES), jnp.int32)
        for s in range(seqs):
            table = jnp.where(row_ids == s, labels_all[s], table)
        col_first = (mine * nz + z) * columns
        local = table - col_first
        code = jnp.where((local >= 0) & (local < columns), local + 1, 0)
        pieces = [code // 16, code % 16, sub_first // 16, sub_first % 16]
        return [piece.astype(jnp.float32).astype(jnp.bfloat16) for piece in pieces]

    def place_labels(pieces, zz):
        ids = nz * iota((rows, LANES), 0) + zz
        member = (ids >= lane_first) & (ids < lane_first + lane_len)
        member = jnp.where(member, 1.0, 0.0).astype(jnp.bfloat16)
        high, low, first_high, first_low = [
            jnp.dot(member, piece, preferred_element_type=jnp.float32) for piece in pieces
        ]
        position = ids.astype(jnp.float32) - (16.0 * first_high + first_low)
        at = position == iota((rows, LANES), 1).astype(jnp.float32)
        code = jnp.sum(jnp.where(at, 16.0 * high + low, 0.0), axis=1, keepdims=True)
        label_place[zz] = jnp.broadcast_to(code - 1.0, (rows, LANES))

    def multiply(chips):
        products = []
        for chip in chips:
            depth = pl.multiple_of((chip // nz) * (2 * LANES), 2 * LANES)
            pair = jnp.concatenate([gathered[0, chip], gathered[1, chip]], axis=1)
            product = jnp.dot(
                pair, weight[pl.ds(depth, 2 * LANES), :], preferred_element_type=jnp.float32
            )
            products.append((chip % nz, product))
        for zz, product in products:
            scores[zz] = scores[zz] + product

    spot = iota((rows, LANES), 1)

    def summarize(zz):
        tiles = [scores[zz, :, k : k + LANES] for k in range(0, columns, LANES)]
        top = jnp.max(functools.reduce(jnp.maximum, tiles), axis=1, keepdims=True)
        total = functools.reduce(jnp.add, [jnp.exp(tile - top) for tile in tiles])
        total = jnp.sum(total, axis=1, keepdims=True)
        code = label_place[zz]
        picked = functools.reduce(
            jnp.add,
            [
                jnp.where(code - float(k * LANES) == spot.astype(jnp.float32), tile, 0.0)
                for k, tile in enumerate(tiles)
            ],
        )
        picked = jnp.sum(picked, axis=1, keepdims=True)
        packed[0:rows, :] = jnp.where(spot == 0, top + jnp.log(total), picked)
        for part in range(parts):
            flat = packed[part * part_rows : part * part_rows + LANES, :].T
            slot = part % pack
            owner = zz * (parts // pack) + part // pack
            stats[owner, slot : slot + 1, :] = flat[0:1, :]
            stats[owner, pack + slot : pack + slot + 1, :] = flat[1:2, :]
            if slot == pack - 1:

                @pl.when(owner != rank)
                def _():
                    pltpu.make_async_remote_copy(
                        src_ref=stats.at[owner],
                        dst_ref=stats_in.at[rank],
                        send_sem=stat_sem.at[0],
                        recv_sem=stat_sem.at[1],
                        device_id=(y, owner // 2, owner % 2, z),
                        device_id_type=MESH,
                    ).start()

    packed[rows:, :] = jnp.zeros((LANES - part_rows, LANES), jnp.float32)
    edges = [0, LANES, rows] if CUTS == 2 else [0, rows]
    plan = gather_plan(dims, CUTS)
    order = {}
    for kind, item, _, _ in plan:
        if kind == "twin":
            order[item] = len(order)

    def piece_ref(node, cut):
        return gathered.at[core, chip_of(node), pl.ds(edges[cut], edges[cut + 1] - edges[cut])]

    def drain(ref, sem):
        pltpu.make_async_copy(ref, ref, sem).wait()

    pieces = None
    first_product = True
    for kind, item, child, way in plan:
        if kind == "wait":
            node, cut = item
            if node != (0, 0, 0):
                drain(piece_ref(node, cut), block_recv.at[order[node] * CUTS + cut])
        elif kind == "twin":
            ref = gathered.at[core, chip_of(item)]
            pltpu.make_async_remote_copy(
                src_ref=ref,
                dst_ref=ref,
                send_sem=twin_send,
                recv_sem=twin_recv.at[order[item]],
                device_id=(y, x, twin, z),
                device_id_type=MESH,
            ).start()
        elif kind == "send":
            node, cut = item
            ref = piece_ref(node, cut)
            step = [0, 0, 0]
            step[way[0]] = way[1] % dims[way[0]]
            ty, tx, tz = shifted(*step)
            pltpu.make_async_remote_copy(
                src_ref=ref,
                dst_ref=ref,
                send_sem=block_send,
                recv_sem=block_recv.at[order[child[0]] * CUTS + cut],
                device_id=(ty, tx, core, tz),
                device_id_type=MESH,
            ).start()
        elif kind == "multiply":
            if first_product:
                load_weight.wait()
                first_product = False
            for node in item:
                drain(gathered.at[twin, chip_of(node)], twin_recv.at[order[node]])
            multiply([chip_of(node) for node in item])
        elif kind == "stats":
            summarize((z + nz - item) % nz)
        else:
            if pieces is None:
                drain(labels_all.at[pl.ds(0, 2 * plane - 1)], label_sem.at[1])
                pieces = label_table()
            place_labels(pieces, (z + nz - item) % nz)

    def merge(ref, slot):
        several = ref[:, slot, :]
        top = jnp.max(several, axis=0, keepdims=True)
        return top + jnp.log(jnp.sum(jnp.exp(several - top), axis=0, keepdims=True))

    pair_ids = iota((LANES, LANES), 0)
    select = jnp.zeros((LANES, LANES), jnp.float32)
    seq_ids = iota((LANES, LANES), 1)
    margins = jnp.zeros((1, LANES), jnp.float32)
    for p in range(pairs):
        hit = jnp.where(seq_ids == pairs_ref[2 * p], 1.0, 0.0)
        hit = hit - jnp.where(seq_ids == pairs_ref[2 * p + 1], 1.0, 0.0)
        select = jnp.where(pair_ids == p, hit, select)
        margins = jnp.where(lane == p, margins_ref[p], margins)
    filled = lane < part_rows
    insides = []
    for slot in range(pack):
        part = rank * pack + slot
        row_ids = nz * ((part % parts) * part_rows + lane) + part // parts
        inside = (row_ids >= sub_first) & (row_ids < sub_first + sub_len)
        inside = jnp.where(inside, 1.0, 0.0)
        by_pair = jnp.dot(select, inside, preferred_element_type=jnp.float32)
        insides.append(jnp.concatenate([inside, by_pair], axis=0))
    contract = (((1,), (1,)), ((), ()))

    stats_in[rank] = stats[rank]
    other_stats = stats_in.at[pl.ds(0, owners - 1)]
    drain(other_stats, stat_sem.at[1])
    merged[...] = jnp.zeros(merged.shape, jnp.float32)
    for slot in range(pack):
        merged[slot : slot + 1, :] = merge(stats_in, slot)
        merged[pack + slot : pack + slot + 1, :] = jnp.sum(
            stats_in[:, pack + slot, :], axis=0, keepdims=True
        )
    sheet = y * nz + z
    merged_in[sheet] = merged[...]
    sheet_peers = sorted(
        [(dy, dz) for dy in range(ny) for dz in range(nz) if (dy, dz) != (0, 0)],
        key=lambda s: -far(s[0], ny) - far(s[1], nz),
    )
    for dy, dz in sheet_peers:
        ty, _, tz = shifted(dy, 0, dz)
        pltpu.make_async_remote_copy(
            src_ref=merged,
            dst_ref=merged_in.at[sheet],
            send_sem=merged_sem.at[0],
            recv_sem=merged_sem.at[1],
            device_id=(ty, x, core, tz),
            device_id_type=MESH,
        ).start()
    other_merged = merged_in.at[pl.ds(0, ny * nz - 1)]
    drain(other_merged, merged_sem.at[1])

    totals = jnp.zeros((1, 2 * LANES), jnp.float32)
    squares = jnp.zeros((1, LANES), jnp.float32)
    for slot in range(pack):
        log_norm = merge(merged_in, slot)
        picked = jnp.sum(merged_in[:, pack + slot, :], axis=0, keepdims=True)
        gain = jnp.where(filled, picked - log_norm, 0.0)
        totals = totals + lax.dot_general(
            jnp.broadcast_to(gain, (8, LANES)),
            insides[slot],
            contract,
            precision=lax.Precision.HIGHEST,
            preferred_element_type=jnp.float32,
        )[0:1, :]
        squares = squares + jnp.where(filled, log_norm * log_norm, 0.0)
    squares = jnp.sum(squares, axis=1, keepdims=True)
    sums[0:1, :] = jnp.where(lane == seqs, squares, totals[:, :LANES])
    sums[1:2, :] = totals[:, LANES:]
    sums_in[rank] = sums[...]
    for dx in sorted(range(nx), key=lambda d: -far(d, nx)):
        for dc in (0, 1):
            if (dx, dc) == (0, 0):
                continue
            _, tx, _ = shifted(0, dx, 0)
            pltpu.make_async_remote_copy(
                src_ref=sums,
                dst_ref=sums_in.at[rank],
                send_sem=sums_sem.at[0],
                recv_sem=sums_sem.at[1],
                device_id=(y, tx, twin if dc else core, z),
                device_id_type=MESH,
            ).start()
    live = functools.reduce(jnp.add, lens).astype(jnp.float32)

    drain(others, parcel_sem.at[0])
    drain(labels_all.at[pl.ds(0, 2 * plane - 1)], label_sem.at[0])
    drain(gathered.at[0, pl.ds(0, plane * nz - 1)], block_send)
    drain(gathered.at[0], twin_send)
    drain(other_stats, stat_sem.at[0])
    drain(other_merged, merged_sem.at[0])
    other_sums = sums_in.at[pl.ds(0, owners - 1)]
    drain(other_sums, sums_sem.at[1])

    table = functools.reduce(jnp.add, [sums_in[k] for k in range(owners)])
    row, difference = table[0:1, :], table[1:2, :]
    score = -pref_beta * (difference - margins)
    pair_row = jnp.maximum(score, 0.0) + log_one_plus(jnp.exp(-jnp.abs(score)))
    z_row = zloss_weight * row / live
    out_ref[0:1, :] = row
    out_ref[1:2, :] = pair_row
    out_ref[2:3, :] = z_row
    out_ref[3:8, :] = jnp.zeros((5, LANES), jnp.float32)
    drain(other_sums, sums_sem.at[0])


def split_results(results_ref, seq_out, pair_out, z_out):
    seqs = seq_out.shape[1]
    seq_out[...] = results_ref[0:1, :seqs]
    pair_out[...] = results_ref[1:2, : pair_out.shape[1]]
    z_out[...] = results_ref[2:3, seqs : seqs + 1]


def per_device(dims, hidden, head_weight, labels, lengths, pair_map, ref_margin):
    ny, nx, nz = dims
    plane = ny * nx
    window, width = hidden.shape
    columns = head_weight.shape[1]
    seqs = lengths.shape[0]
    live = seqs * window // 2
    rows = live // nz
    slots = -(-window // (nz * 16)) * 16
    bf16, f32, i32 = jnp.bfloat16, jnp.float32, jnp.int32
    vmem = pltpu.VMEM
    dma = pltpu.SemaphoreType.DMA
    results = pl.pallas_call(
        functools.partial(kernel, dims),
        out_shape=jax.ShapeDtypeStruct((8, LANES), f32),
        in_specs=[
            pl.BlockSpec(memory_space=pl.ANY),
        ]
        * 6,
        out_specs=pl.BlockSpec(memory_space=vmem),
        scratch_shapes=[
            vmem((1, window), i32),
            pltpu.SMEM((seqs,), i32),
            pltpu.SMEM((seqs,), i32),
            pltpu.SMEM((seqs // 2,), f32),
            vmem((window, width), bf16),
            vmem((width, columns), bf16),
            vmem((2 * plane, slots, LANES), bf16),
            vmem((2 * plane, slots, LANES), bf16),
            vmem((1, LANES), i32),
            vmem((2 * plane, 1, LANES), i32),
            vmem((2, plane * nz, rows, LANES), bf16),
            vmem((nz, rows, columns), f32),
            vmem((nz, rows, LANES), f32),
            vmem((rows + LANES // 16, LANES), f32),
            vmem((2 * nx, 4, LANES), f32),
            vmem((2 * nx, 4, LANES), f32),
            vmem((4, LANES), f32),
            vmem((ny * nz, 4, LANES), f32),
            vmem((2, LANES), f32),
            vmem((2 * nx, 2, LANES), f32),
            dma((6,)),
            dma((2,)),
            dma((2,)),
            dma(()),
            dma(()),
            dma((CUTS * plane * nz,)),
            dma((plane * nz,)),
            dma((2,)),
            dma((2,)),
            dma((2,)),
        ],
        compiler_params=pltpu.CompilerParams(collective_id=0, has_side_effects=True),
    )(hidden, head_weight, labels.reshape(1, window), lengths, pair_map, ref_margin)
    seq_logps, pair_loss, z_loss = pl.pallas_call(
        split_results,
        out_shape=[jax.ShapeDtypeStruct((1, n), f32) for n in (seqs, seqs // 2, 1)],
        in_specs=[pl.BlockSpec(memory_space=vmem)],
        out_specs=[pl.BlockSpec(memory_space=vmem)] * 3,
    )(results)
    return seq_logps.reshape(seqs), pair_loss.reshape(seqs // 2), z_loss.reshape(())


def solution(mesh):
    nz = mesh.shape["vocab"]
    ny = nx = {32: 4, 8: 2}[mesh.shape["seq"]]
    torus = Mesh(
        mesh.devices.reshape(ny, nx, 2, nz), ("seq_0", "seq_1", "seq_2", "vocab")
    )
    return jax.shard_map(
        functools.partial(per_device, (ny, nx, nz)),
        mesh=torus,
        in_specs=(P(SEQ, None), P(None, SEQ_VOCAB), P(SEQ), P(), P(), P()),
        out_specs=(P(), P(), P()),
        check_vma=False,
    )
```
